32 devices in a mesh: comm: 4 (over y, x), wide: 8 (over z, core).
Axes of the slice: x: 2, y: 2, z: 4, core: 2. Of those that a mesh axis runs over, the one named last changes fastest.
Arguments:
- feats: bfloat16 [64, 768, 768], P(('comm', 'wide')), may hold values from -6 to 6
- tiles: bfloat16 [64, 3, 768, 768], P(('comm', 'wide')), may hold values from -0.15625 to 0.15625
- tile_src: int32 [64, 3], P(('comm', 'wide')), may hold values from 0 to 5
- tile_count: int32 [64], P(('comm', 'wide')), may hold values from 1 to 3
- request: int32 [32, 4], P(('comm', 'wide')), may hold values from 0 to 1
- z_old: bfloat16 [64, 768, 1024], P(('comm', 'wide')), may hold values from -6 to 6
- dual: bfloat16 [64, 768, 1024], P(('comm', 'wide')), may hold values from -6 to 6
- target: bfloat16 [64, 768, 1024], P(('comm', 'wide')), may hold values from 0 to 2
- w_rows: bfloat16 [768, 1024], P('wide'), may hold values from -0.21875 to 0.21875
- rho: float32 [1024], replicated, may hold values from 0.3 to 4
- beta: float32 [1024], replicated, may hold values from 0.3 to 4
Outputs:
- new_z: bfloat16 [64, 768, 1024], P(('comm', 'wide'))
- new_dual: bfloat16 [64, 768, 1024], P(('comm', 'wide'))
- weight_grad: float32 [768, 1024], P('wide')
The draws below stay inside these ranges and needn't reach their ends.
Inputs may be any that keep to these rules, and one draw needn't show every extreme that they name: `tile_src`: entries beyond tile_count of a community are not read.
All inputs are finite; a program needn't handle non-finite values.
Results may differ from the reference program's by a relative error of at most 0.0095.
Values may be sent and summed in bfloat16 or wider, within the bound.
A program may use at most 128 MiB of HBM per device.

```python
import math
import jax
import jax.numpy as jnp
from jax import lax

C = 768
F = 768
H = 1024
TILES = 3
COMM_DEV = 2
COMMS = 64
NODES = 49152
N_COMM = 4
N_WIDE = 8
DEVICES = 32


def plant(result, rng, low, high):
    shape = result.shape
    place = [jax.random.randint(jax.random.fold_in(rng, axis), (), 0, shape[axis]) for axis in range(len(shape))]
    result = result.at[tuple(place)].set(low)
    longest = shape.index(max(shape))
    place[longest] = (place[longest] + 1) % shape[longest]
    return result.at[tuple(place)].set(high)


def shard_levels(own_key, shape, pieces, low, largest):
    def one(dim, shards_of):
        draws = jax.random.uniform(jax.random.fold_in(jax.random.fold_in(own_key, 6), dim), (shards_of,), jnp.float32, low / len(pieces), largest / len(pieces))
        return jnp.repeat(jnp.exp(draws), shape[dim] // shards_of).reshape((-1,) + (1,) * (len(shape) - dim - 1))

    factor_of = one(*pieces[0])
    for cut in pieces[1:]:
        factor_of = factor_of * one(*cut)
    return factor_of


def gaussian(key, shape, spread, most, shards=(), kind=jnp.bfloat16):
    values = jax.random.normal(key, shape, jnp.float32) * spread
    if len(shards) > 0:
        values = shard_levels(key, shape, shards, -0.22, 0.18) * values
    return jnp.clip(values, min=-most, max=most).astype(kind)


def setup_inputs(seed: int = 0) -> dict:
    keys = jax.random.split(jax.random.key(seed), 12)
    return {
        "feats": gaussian(keys[0], (COMMS, C, F), 1.0, 6.0, ((0, 32),)),
        "tiles": gaussian(keys[1], (COMMS, TILES, C, C), (C * 2) ** -0.5, 0.15625, ((0, 32),)),
        "tile_src": plant(jax.random.randint(keys[2], (COMMS, TILES), 0, COMM_DEV + N_COMM), jax.random.fold_in(keys[2], 1), 0, (COMM_DEV + N_COMM) - 1).astype(jnp.int32),
        "tile_count": plant(jax.random.randint(keys[3], (COMMS,), 1, TILES + 1), jax.random.fold_in(keys[3], 1), 1, TILES).astype(jnp.int32),
        "request": plant(jax.random.randint(keys[4], (DEVICES, N_COMM), 0, COMM_DEV), jax.random.fold_in(keys[4], 1), 0, COMM_DEV - 1).astype(jnp.int32),
        "z_old": gaussian(keys[5], (COMMS, C, H), 1.0, 6.0, ((0, 32),)),
        "dual": gaussian(keys[6], (COMMS, C, H), 1.0, 6.0, ((0, 32),)),
        "target": jnp.clip(2.0 * jax.random.uniform(keys[7], (COMMS, C, H), jnp.float32) ** shard_levels(keys[7], (COMMS, C, H), ((0, 32),), -0.2, 0.2), 0.0, 2.0).astype(jnp.bfloat16),
        "w_rows": gaussian(keys[8], (F, H), F ** -0.5, 0.21875, ((0, 8),)),
        "rho": jnp.clip(jnp.exp(jax.random.uniform(keys[9], (H,), jnp.float32, math.log(0.3), math.log(4.0))), 0.3, 4.0),
        "beta": jnp.clip(jnp.exp(jax.random.uniform(keys[10], (H,), jnp.float32, math.log(0.3), math.log(4.0))), 0.3, 4.0),
    }


def reference(feats, tiles, tile_src, tile_count, request, z_old, dual, target, w_rows, rho, beta):
    owner = jnp.arange(COMMS, dtype=jnp.int32) // COMM_DEV
    wide_pos = owner % N_WIDE
    slot = jnp.maximum(tile_src - COMM_DEV, 0).astype(jnp.int32)
    peer_dev = slot * N_WIDE + wide_pos[:, None]
    picked = request[owner[:, None], slot]
    remote = peer_dev * COMM_DEV + picked
    local = owner[:, None] * COMM_DEV + tile_src
    source = jnp.where(tile_src < COMM_DEV, local, remote).astype(jnp.int32)
    live = (jnp.arange(TILES, dtype=jnp.int32)[None, :] < tile_count[:, None]).astype(jnp.float32)

    def one(args):
        tile_set, index, keep = args
        blocks = feats[index].astype(jnp.float32) * keep[:, None, None]
        total = jnp.einsum('tij,tjf->if', tile_set.astype(jnp.float32), blocks)
        return total.astype(jnp.bfloat16)
    agg = lax.map(one, (tiles, source, live))
    flat = agg.reshape(-1, F)
    pre = jnp.dot(flat, w_rows, preferred_element_type=jnp.float32).reshape(COMMS, C, H)
    shifted = pre + dual.astype(jnp.float32) / rho
    active = (rho * shifted + beta * target.astype(jnp.float32)) / (rho + beta)
    znew = jnp.where(z_old > 0, active, shifted)
    new_dual = (dual.astype(jnp.float32) + rho * (pre - znew)).astype(jnp.bfloat16)
    grad = jnp.einsum('nf,nh->fh', flat.astype(jnp.float32), new_dual.reshape(-1, H).astype(jnp.float32))
    grad = grad * (1.0 / math.sqrt(NODES))
    return (znew.astype(jnp.bfloat16), new_dual, grad)
```

```python
import functools
import math

import jax
import jax.numpy as jnp
from jax import lax
from jax.experimental import pallas as pl
from jax.experimental.pallas import tpu as pltpu
from jax.sharding import PartitionSpec as P


VMEM_BYTES = 60 * 1024 * 1024

MESH = pl.DeviceIdType.MESH


def largest_block(size, limit, unit):
    for block in range(limit, 0, -unit):
        if size % block == 0:
            return block
    return size


def mxu(a, b):
    return jnp.dot(a, b, preferred_element_type=jnp.float32)


def step_kernel(n_comm, n_wide, plan, *refs):
    (chunks, cw, rows, tail_rows, column, gather_w) = plan
    (src_ref, count_ref, request_ref, feats_ref, tiles_ref, z_ref, dual_ref, target_ref, w_ref, rho_ref,
     beta_ref, newz_ref, newdual_ref, grad_ref, own, tiles, z_old, dual, target, weight, part, agg_t,
     ask, asked) = refs[:24]
    pools = refs[24 : 24 + chunks]
    stages = refs[24 + chunks : 24 + 2 * chunks]
    (own_sem, pool_sem, tile_sem, data_sem, w_sem, ask_send, ask_recv, feat_send, feat_recv, w_send, w_recv,
     fwd_send, fwd_recv) = refs[24 + 2 * chunks :]
    own_count, nodes, width = feats_ref.shape
    slots = tiles_ref.shape[1]
    hidden = w_ref.shape[-1]
    peers = n_comm - 1
    paired = n_comm & (n_comm - 1) == 0
    half = n_wide // 2
    dead = own_count + peers
    c = lax.axis_index("comm")
    w = lax.axis_index("wide")
    chip = w // 2
    side = lax.rem(w, 2)
    partner = w + 1 - 2 * side

    def towards(off):
        return lax.bitwise_xor(c, off) if paired else lax.rem(c + off, n_comm)

    def arriving(off):
        return lax.bitwise_xor(c, off) if paired else lax.rem(c - off + n_comm, n_comm)

    def along(off):
        return lax.rem(chip + off, half) * 2 + side

    own_copy = pltpu.make_async_copy(feats_ref, own, own_sem.at[0])
    own_copy.start()
    if gather_w:
        w_copy = pltpu.make_async_copy(w_ref, weight.at[w], w_sem.at[0])
    else:
        w_copy = pltpu.make_async_copy(w_ref, weight, w_sem.at[0])
    w_copy.start()
    pool_copies = []
    for j in range(chunks):
        pool_copies.append(
            pltpu.make_async_copy(
                feats_ref.at[:, :, pl.ds(j * cw, cw)], pools[j].at[pl.ds(0, own_count)], pool_sem.at[j]
            )
        )
    tile_copy = pltpu.make_async_copy(tiles_ref, tiles, tile_sem.at[0])
    data_copies = [
        pltpu.make_async_copy(dual_ref, dual, data_sem.at[0]),
        pltpu.make_async_copy(target_ref, target, data_sem.at[1]),
        pltpu.make_async_copy(z_ref, z_old, data_sem.at[2]),
    ]

    def signal(to_c, to_w):
        pl.semaphore_signal(
            pltpu.get_barrier_semaphore(), inc=1, device_id=(to_c, to_w), device_id_type=MESH
        )

    def remote(src, dst, send, recv, to_c, to_w):
        return pltpu.make_async_remote_copy(
            src_ref=src, dst_ref=dst, send_sem=send, recv_sem=recv, device_id=(to_c, to_w),
            device_id_type=MESH,
        )

    def arrived(dst, recv):
        remote(dst, dst, recv, recv, c, partner).wait_recv()

    for off in range(1, n_comm):
        signal(lax.rem(c + off, n_comm), w)
    greeted = peers
    if gather_w:
        for off in range(1, half):
            signal(c, along(off))
        signal(c, partner)
        greeted += half
    for off in range(1, n_comm):
        ask[off - 1] = jnp.full(ask.shape[1:], request_ref[0, arriving(off)], jnp.int32)
    pl.semaphore_wait(pltpu.get_barrier_semaphore(), greeted)

    started = []

    def start(*args):
        copy = remote(*args)
        copy.start()
        started.append(copy)

    order = [peers] + list(range(1, peers))
    for off in order:
        start(ask.at[off - 1], asked.at[off - 1], ask_send.at[off - 1], ask_recv.at[off - 1], arriving(off), w)
    for copy in pool_copies:
        copy.start()
    tile_copy.start()
    for copy in data_copies:
        copy.start()
    w_copy.wait()
    if gather_w:
        for off in range(1, half):
            start(weight.at[w], weight.at[w], w_send.at[off - 1], w_recv.at[chip], c, along(off))
        start(weight.at[w], weight.at[w], fwd_send.at[0], fwd_recv.at[chip], c, partner)
    own_copy.wait()
    wants = {}
    for j in range(chunks):
        for off in order:
            if j == 0:
                arrived(asked.at[off - 1], ask_recv.at[off - 1])
                wants[off] = jnp.clip(jnp.max(asked[off - 1]), 0, own_count - 1)
            stages[j][off - 1] = own[wants[off], :, j * cw : (j + 1) * cw]
            start(
                stages[j].at[off - 1], pools[j].at[own_count + off - 1], feat_send.at[off - 1, j],
                feat_recv.at[off - 1, j], towards(off), w,
            )
    for j in range(chunks):
        pools[j][dead] = jnp.zeros((nodes, cw), jnp.bfloat16)

    def pick(k, t):
        source = src_ref[k, t]
        member = jnp.maximum(source - own_count, 0)
        if paired:
            offset = lax.bitwise_xor(c, member)
        else:
            offset = lax.rem(c - member + n_comm, n_comm)
        other = jnp.where(member == c, request_ref[0, c], own_count + offset - 1)
        index = jnp.where(source < own_count, source, other)
        index = jnp.clip(index, 0, dead - 1)
        return jnp.where(t < count_ref[k], index, dead)

    rho = rho_ref[...]
    beta = beta_ref[...]
    inverse = 1.0 / rho
    blend = beta / (rho + beta)
    gain = rho * blend

    def gathered(j, k, at, size):
        block = pl.ds(pl.multiple_of(at * size, size), size)
        total = mxu(tiles[k, 0, block, :], pools[j][pick(k, 0)])
        for t in range(1, slots):
            total = total + mxu(tiles[k, t, block, :], pools[j][pick(k, t)])
        agg = total.astype(jnp.bfloat16)
        column_at = pl.multiple_of(k * nodes + at * size, 128)
        agg_t[j * cw : (j + 1) * cw, pl.ds(column_at, size)] = agg.T
        return agg, block

    if gather_w:
        for off in range(1, half):
            other = along(off)
            arrived(weight.at[other], w_recv.at[other // 2])
            start(weight.at[other], weight.at[other], fwd_send.at[off], fwd_recv.at[other // 2], c, partner)
        for at in range(half):
            arrived(weight.at[at * 2 + 1 - side], fwd_recv.at[at])
    tile_copy.wait()
    for copy in data_copies:
        copy.wait()

    def w_part(j, at):
        cols = slice(at * column, (at + 1) * column)
        if gather_w:
            shard = weight.shape[1]
            return weight[...].reshape(width, hidden)[j * cw : (j + 1) * cw, cols]
        return weight[j * cw : (j + 1) * cw, cols]

    for j in range(chunks):
        pool_copies[j].wait()
        for off in order:
            arrived(pools[j].at[own_count + off - 1], feat_recv.at[off - 1, j])
        if j < chunks - 1:
            steps = nodes // rows

            def body(step, carry, j=j, steps=steps):
                k = step // steps
                agg, block = gathered(j, k, lax.rem(step, steps), rows)
                for at in range(hidden // column):
                    cols = slice(at * column, (at + 1) * column)
                    value = mxu(agg, w_part(j, at))
                    if j == 0:
                        value = value + (
                            dual[k, block, cols].astype(jnp.float32) * inverse[:, cols]
                            - target[k, block, cols].astype(jnp.float32)
                        )
                    else:
                        value = value + part[k, block, cols]
                    part[k, block, cols] = value
                return carry

            lax.fori_loop(0, own_count * steps, body, 0)
        else:
            steps = nodes // tail_rows

            def tail(step, carry, j=j, steps=steps):
                k = step // steps
                agg, block = gathered(j, k, lax.rem(step, steps), tail_rows)
                for at in range(hidden // column):
                    cols = slice(at * column, (at + 1) * column)
                    gap = mxu(agg, w_part(j, at)) + part[k, block, cols]
                    moved = jnp.where(z_old[k, block, cols].astype(jnp.float32) > 0, gap, 0.0)
                    newdual_ref[k, block, cols] = (gain[:, cols] * moved).astype(jnp.bfloat16)
                    newz_ref[k, block, cols] = (
                        gap + target[k, block, cols].astype(jnp.float32) - blend[:, cols] * moved
                    ).astype(jnp.bfloat16)
                return carry

            lax.fori_loop(0, own_count * steps, tail, 0)

    fb = grad_ref.shape[0] // chunks

    def gradient(step, carry):
        block = pl.ds(pl.multiple_of(step * fb, fb), fb)
        for at in range(hidden // column):
            cols = slice(at * column, (at + 1) * column)
            moved = newdual_ref[:, :, cols].reshape(own_count * nodes, column)
            grad_ref[block, cols] = mxu(agg_t[block, :], moved).astype(jnp.bfloat16)
        return carry

    lax.fori_loop(0, chunks, gradient, 0)
    for copy in started:
        copy.wait_send()


def step(tile_src, tile_count, request, feats, tiles, z_old, dual, target, w_rows, rho, beta, n_comm, n_wide):
    own_count, nodes, width = feats.shape
    slots = tiles.shape[1]
    hidden = w_rows.shape[1]
    gather_w = w_rows.shape[0] % 16 == 0
    if not gather_w:
        w_rows = lax.all_gather(w_rows, "wide", axis=0, tiled=True)
    cw = largest_block(width, 256, 128)
    chunks = width // cw
    column = largest_block(hidden, 256, 128)
    rows = largest_block(nodes, 384, 128)
    tail_rows = largest_block(nodes, 256, 128)
    plan = (chunks, cw, rows, tail_rows, column, gather_w)
    peers = n_comm - 1
    half = n_wide // 2
    bf16 = jnp.bfloat16
    smem = pl.BlockSpec(memory_space=pltpu.SMEM)
    vmem = pl.BlockSpec(memory_space=pltpu.VMEM)
    anywhere = pl.BlockSpec(memory_space=pl.ANY)
    dma = pltpu.SemaphoreType.DMA
    weight = pltpu.VMEM((n_wide,) + w_rows.shape if gather_w else w_rows.shape, bf16)
    return pl.pallas_call(
        functools.partial(step_kernel, n_comm, n_wide, plan),
        out_shape=[
            jax.ShapeDtypeStruct(z_old.shape, bf16),
            jax.ShapeDtypeStruct(dual.shape, bf16),
            jax.ShapeDtypeStruct((width, hidden), bf16),
        ],
        in_specs=[smem] * 3 + [anywhere] * 6 + [vmem] * 2,
        out_specs=[vmem] * 3,
        scratch_shapes=[
            pltpu.VMEM(feats.shape, bf16),
            pltpu.VMEM(tiles.shape, bf16),
            pltpu.VMEM(z_old.shape, bf16),
            pltpu.VMEM(dual.shape, bf16),
            pltpu.VMEM(target.shape, bf16),
            weight,
            pltpu.VMEM(z_old.shape, jnp.float32),
            pltpu.VMEM((width, own_count * nodes), bf16),
            pltpu.VMEM((peers, 8, 128), jnp.int32),
            pltpu.VMEM((peers, 8, 128), jnp.int32),
        ]
        + [pltpu.VMEM((own_count + n_comm, nodes, cw), bf16)] * chunks
        + [pltpu.VMEM((peers, nodes, cw), bf16)] * chunks
        + [
            dma((1,)), dma((chunks,)), dma((1,)), dma((3,)), dma((1,)), dma((peers,)), dma((peers,)),
            dma((peers, chunks)), dma((peers, chunks)), dma((half,)), dma((half,)), dma((half,)), dma((half,)),
        ],
        compiler_params=pltpu.CompilerParams(
            collective_id=1, has_side_effects=True, vmem_limit_bytes=VMEM_BYTES
        ),
        cost_estimate=pl.CostEstimate(flops=1 << 36, bytes_accessed=32 << 20, transcendentals=0),
    )(tile_src, tile_count, request, feats, tiles, z_old, dual, target, w_rows, rho, beta)


def reduce_kernel(
    n_comm, n_wide, factor, grad_ref, out_ref, got_pair, sums, got_comm, parts, got_wide, final,
    pair_send, pair_recv, comm_send, comm_recv, wide_send, wide_recv, final_send, final_recv,
):
    half = n_wide // 2
    columns = sums.shape[-1]
    c = lax.axis_index("comm")
    w = lax.axis_index("wide")
    mine = w // 2
    side = lax.rem(w, 2)
    partner = w + 1 - 2 * side

    def signal(to_c, to_w):
        pl.semaphore_signal(
            pltpu.get_barrier_semaphore(),
            inc=1,
            device_id=(to_c, to_w),
            device_id_type=pl.DeviceIdType.MESH,
        )

    signal(c, partner)
    for off in range(1, half):
        signal(c, lax.rem(mine + off, half) * 2 + side)
    for off in range(1, n_comm):
        signal(lax.rem(c + off, n_comm), w)
    pl.semaphore_wait(pltpu.get_barrier_semaphore(), 1 + (half - 1) + (n_comm - 1))

    def remote(src, dst, send, recv, to_c, to_w):
        return pltpu.make_async_remote_copy(
            src_ref=src,
            dst_ref=dst,
            send_sem=send,
            recv_sem=recv,
            device_id=(to_c, to_w),
            device_id_type=pl.DeviceIdType.MESH,
        )

    def arrived(dst, recv):
        remote(dst, dst, recv, recv, c, partner).wait_recv()

    started = []

    def start(*args):
        copy = remote(*args)
        copy.start()
        started.append(copy)

    order = [lax.rem(mine + off, half) for off in range(1, half)] + [mine]
    for at, j in enumerate(order):
        start(
            grad_ref.at[2 * j + 1 - side], got_pair.at[at], pair_send.at[at], pair_recv.at[at],
            c, partner,
        )
    for at, j in enumerate(order):
        arrived(got_pair.at[at], pair_recv.at[at])
        value = grad_ref[2 * j + side].astype(jnp.float32) + got_pair[at].astype(jnp.float32)
        value = value.astype(jnp.bfloat16)
        for q in range(n_comm):
            sums[q, at] = value[:, q * columns : (q + 1) * columns]
        for off in range(1, n_comm):
            q = lax.rem(c + off, n_comm)
            start(
                sums.at[q, at], got_comm.at[c, at], comm_send.at[off - 1, at],
                comm_recv.at[c, at], q, w,
            )
    for at, j in enumerate(order):
        value = sums[c, at].astype(jnp.float32)
        for off in range(1, n_comm):
            q = lax.rem(c + off, n_comm)
            arrived(got_comm.at[q, at], comm_recv.at[q, at])
            value = value + got_comm[q, at].astype(jnp.float32)
        if at < half - 1:
            parts[at] = value.astype(jnp.bfloat16)
            start(
                parts.at[at], got_wide.at[mine], wide_send.at[at], wide_recv.at[mine],
                c, j * 2 + side,
            )
        else:
            total = value
    for off in range(1, half):
        j = lax.rem(mine + off, half)
        arrived(got_wide.at[j], wide_recv.at[j])
        total = total + got_wide[j].astype(jnp.float32)
    final[c] = total.astype(jnp.bfloat16)
    for off in range(1, n_comm):
        start(
            final.at[c], final.at[c], final_send.at[off - 1], final_recv.at[c],
            lax.rem(c + off, n_comm), w,
        )
    for off in range(1, n_comm):
        q = lax.rem(c + off, n_comm)
        arrived(final.at[q], final_recv.at[q])
    for q in range(n_comm):
        out_ref[:, q * columns : (q + 1) * columns] = final[q].astype(jnp.float32) * factor
    for copy in started:
        copy.wait_send()


def reduce_grad(grad, n_comm, n_wide, factor):
    width, hidden = grad.shape
    rows = width // n_wide
    half = n_wide // 2
    block = (rows, hidden)
    piece = (rows, hidden // n_comm)
    return pl.pallas_call(
        functools.partial(reduce_kernel, n_comm, n_wide, factor),
        out_shape=jax.ShapeDtypeStruct(block, jnp.float32),
        in_specs=[pl.BlockSpec(memory_space=pltpu.VMEM)],
        out_specs=pl.BlockSpec(memory_space=pltpu.VMEM),
        scratch_shapes=[
            pltpu.VMEM((half,) + block, jnp.bfloat16),
            pltpu.VMEM((n_comm, half) + piece, jnp.bfloat16),
            pltpu.VMEM((n_comm, half) + piece, jnp.bfloat16),
            pltpu.VMEM((half,) + piece, jnp.bfloat16),
            pltpu.VMEM((half,) + piece, jnp.bfloat16),
            pltpu.VMEM((n_comm,) + piece, jnp.bfloat16),
            pltpu.SemaphoreType.DMA((half,)),
            pltpu.SemaphoreType.DMA((half,)),
            pltpu.SemaphoreType.DMA((n_comm, half)),
            pltpu.SemaphoreType.DMA((n_comm, half)),
            pltpu.SemaphoreType.DMA((half,)),
            pltpu.SemaphoreType.DMA((half,)),
            pltpu.SemaphoreType.DMA((n_comm,)),
            pltpu.SemaphoreType.DMA((n_comm,)),
        ],
        compiler_params=pltpu.CompilerParams(collective_id=0, has_side_effects=True),
    )(grad.reshape((n_wide,) + block))


def local(feats, tiles, tile_src, tile_count, request, z_old, dual, target, w_rows, rho, beta):
    own_count, nodes, _ = feats.shape
    hidden = w_rows.shape[1]
    n_comm = lax.axis_size("comm")
    n_wide = lax.axis_size("wide")
    new_z, new_dual, grad = step(
        tile_src, tile_count, request, feats, tiles, z_old, dual, target, w_rows,
        rho.reshape(1, hidden), beta.reshape(1, hidden), n_comm, n_wide,
    )
    factor = 1.0 / math.sqrt(own_count * nodes * n_comm * n_wide)
    return new_z, new_dual, reduce_grad(grad, n_comm, n_wide, factor)


def solution(mesh):
    in_specs = (
        P(("comm", "wide"), None, None),
        P(("comm", "wide"), None, None, None),
        P(("comm", "wide"), None),
        P(("comm", "wide")),
        P(("comm", "wide"), None),
        P(("comm", "wide"), None, None),
        P(("comm", "wide"), None, None),
        P(("comm", "wide"), None, None),
        P("wide", None),
        P(),
        P(),
    )
    out_specs = (P(("comm", "wide"), None, None), P(("comm", "wide"), None, None), P("wide", None))
    return jax.shard_map(local, mesh=mesh, in_specs=in_specs, out_specs=out_specs, check_vma=False)
```

```python
import functools
import math

import jax
import jax.numpy as jnp
from jax import lax
from jax.experimental import pallas as pl
from jax.experimental.pallas import tpu as pltpu
from jax.sharding import PartitionSpec as P


STEP_VMEM = 46 * 1024 * 1024

REDUCE_VMEM = 10 * 1024 * 1024

MESH = pl.DeviceIdType.MESH


def largest_block(size, limit, unit):
    for block in range(limit, 0, -unit):
        if size % block == 0:
            return block
    return size


def mxu(a, b):
    return jnp.dot(a, b, preferred_element_type=jnp.float32)


def step_kernel(n_comm, n_wide, plan, *refs):
    (chunks, cw, rows, tail_rows, column, gather_w) = plan
    (src_ref, count_ref, request_ref, feats_ref, tiles_ref, z_ref, dual_ref, target_ref, w_ref, rho_ref,
     beta_ref, newz_ref, newdual_ref, agg_t, own, tiles, z_old, dual, target, weight, part,
     ask, asked) = refs[:23]
    pools = refs[23 : 23 + chunks]
    stages = refs[23 + chunks : 23 + 2 * chunks]
    (own_sem, pool_sem, tile_sem, data_sem, w_sem, ask_send, ask_recv, feat_send, feat_recv, w_send, w_recv,
     fwd_send, fwd_recv) = refs[23 + 2 * chunks :]
    own_count, nodes, width = feats_ref.shape
    slots = tiles_ref.shape[1]
    hidden = w_ref.shape[-1]
    peers = n_comm - 1
    paired = n_comm & (n_comm - 1) == 0
    half = n_wide // 2
    dead = own_count + peers
    c = lax.axis_index("comm")
    w = lax.axis_index("wide")
    chip = w // 2
    side = lax.rem(w, 2)
    partner = w + 1 - 2 * side

    def towards(off):
        return lax.bitwise_xor(c, off) if paired else lax.rem(c + off, n_comm)

    def arriving(off):
        return lax.bitwise_xor(c, off) if paired else lax.rem(c - off + n_comm, n_comm)

    def along(off):
        return lax.rem(chip + off, half) * 2 + side

    own_copy = pltpu.make_async_copy(feats_ref, own, own_sem.at[0])
    own_copy.start()
    if gather_w:
        w_copy = pltpu.make_async_copy(w_ref, weight.at[w], w_sem.at[0])
    else:
        w_copy = pltpu.make_async_copy(w_ref, weight, w_sem.at[0])
    w_copy.start()
    pool_copies = []
    for j in range(chunks):
        pool_copies.append(
            pltpu.make_async_copy(
                feats_ref.at[:, :, pl.ds(j * cw, cw)], pools[j].at[pl.ds(0, own_count)], pool_sem.at[j]
            )
        )
    tile_copy = pltpu.make_async_copy(tiles_ref, tiles, tile_sem.at[0])
    data_copies = [
        pltpu.make_async_copy(dual_ref, dual, data_sem.at[0]),
        pltpu.make_async_copy(target_ref, target, data_sem.at[1]),
        pltpu.make_async_copy(z_ref, z_old, data_sem.at[2]),
    ]

    def signal(to_c, to_w):
        pl.semaphore_signal(
            pltpu.get_barrier_semaphore(), inc=1, device_id=(to_c, to_w), device_id_type=MESH
        )

    def remote(src, dst, send, recv, to_c, to_w):
        return pltpu.make_async_remote_copy(
            src_ref=src, dst_ref=dst, send_sem=send, recv_sem=recv, device_id=(to_c, to_w),
            device_id_type=MESH,
        )

    def arrived(dst, recv):
        remote(dst, dst, recv, recv, c, partner).wait_recv()

    for off in range(1, n_comm):
        signal(lax.rem(c + off, n_comm), w)
    greeted = peers
    if gather_w:
        for off in range(1, half):
            signal(c, along(off))
        signal(c, partner)
        greeted += half
    for off in range(1, n_comm):
        ask[off - 1] = jnp.full(ask.shape[1:], request_ref[0, arriving(off)], jnp.int32)
    pl.semaphore_wait(pltpu.get_barrier_semaphore(), greeted)

    started = []

    def start(*args):
        copy = remote(*args)
        copy.start()
        started.append(copy)

    order = [peers] + list(range(1, peers))
    for off in order:
        start(ask.at[off - 1], asked.at[off - 1], ask_send.at[off - 1], ask_recv.at[off - 1], arriving(off), w)
    for copy in pool_copies:
        copy.start()
    tile_copy.start()
    for copy in data_copies:
        copy.start()
    w_copy.wait()
    if gather_w:
        for off in range(1, half):
            start(weight.at[w], weight.at[w], w_send.at[off - 1], w_recv.at[chip], c, along(off))
        start(weight.at[w], weight.at[w], fwd_send.at[0], fwd_recv.at[chip], c, partner)
    own_copy.wait()
    wants = {}
    for j in range(chunks):
        for off in order:
            if j == 0:
                arrived(asked.at[off - 1], ask_recv.at[off - 1])
                wants[off] = jnp.clip(jnp.max(asked[off - 1]), 0, own_count - 1)
            stages[j][off - 1] = own[wants[off], :, j * cw : (j + 1) * cw]
            start(
                stages[j].at[off - 1], pools[j].at[own_count + off - 1], feat_send.at[off - 1, j],
                feat_recv.at[off - 1, j], towards(off), w,
            )
    for j in range(chunks):
        pools[j][dead] = jnp.zeros((nodes, cw), jnp.bfloat16)

    def pick(k, t):
        source = src_ref[k, t]
        member = jnp.maximum(source - own_count, 0)
        if paired:
            offset = lax.bitwise_xor(c, member)
        else:
            offset = lax.rem(c - member + n_comm, n_comm)
        other = jnp.where(member == c, request_ref[0, c], own_count + offset - 1)
        index = jnp.where(source < own_count, source, other)
        index = jnp.clip(index, 0, dead - 1)
        return jnp.where(t < count_ref[k], index, dead)

    rho = rho_ref[...]
    beta = beta_ref[...]
    inverse = 1.0 / rho
    blend = beta / (rho + beta)
    gain = rho * blend

    def gathered(j, k, at, size):
        block = pl.ds(pl.multiple_of(at * size, size), size)
        total = mxu(tiles[k, 0, block, :], pools[j][pick(k, 0)])
        for t in range(1, slots):
            total = total + mxu(tiles[k, t, block, :], pools[j][pick(k, t)])
        agg = total.astype(jnp.bfloat16)
        column_at = pl.multiple_of(k * nodes + at * size, 128)
        agg_t[j * cw : (j + 1) * cw, pl.ds(column_at, size)] = agg.T
        return agg, block

    if gather_w:
        for off in range(1, half):
            other = along(off)
            arrived(weight.at[other], w_recv.at[other // 2])
            start(weight.at[other], weight.at[other], fwd_send.at[off], fwd_recv.at[other // 2], c, partner)
        for at in range(half):
            arrived(weight.at[at * 2 + 1 - side], fwd_recv.at[at])
    tile_copy.wait()
    for copy in data_copies:
        copy.wait()

    def w_part(j, at):
        cols = slice(at * column, (at + 1) * column)
        if gather_w:
            shard = weight.shape[1]
            return weight[...].reshape(width, hidden)[j * cw : (j + 1) * cw, cols]
        return weight[j * cw : (j + 1) * cw, cols]

    for j in range(chunks):
        pool_copies[j].wait()
        for off in order:
            arrived(pools[j].at[own_count + off - 1], feat_recv.at[off - 1, j])
        if j < chunks - 1:
            steps = nodes // rows

            def body(step, carry, j=j, steps=steps):
                k = step // steps
                agg, block = gathered(j, k, lax.rem(step, steps), rows)
                for at in range(hidden // column):
                    cols = slice(at * column, (at + 1) * column)
                    value = mxu(agg, w_part(j, at))
                    if j == 0:
                        value = value + (
                            dual[k, block, cols].astype(jnp.float32) * inverse[:, cols]
                            - target[k, block, cols].astype(jnp.float32)
                        )
                    else:
                        value = value + part[k, block, cols]
                    part[k, block, cols] = value
                return carry

            lax.fori_loop(0, own_count * steps, body, 0)
        else:
            steps = nodes // tail_rows

            def tail(step, carry, j=j, steps=steps):
                k = step // steps
                agg, block = gathered(j, k, lax.rem(step, steps), tail_rows)
                for at in range(hidden // column):
                    cols = slice(at * column, (at + 1) * column)
                    gap = mxu(agg, w_part(j, at)) + part[k, block, cols]
                    moved = jnp.where(z_old[k, block, cols].astype(jnp.float32) > 0, gap, 0.0)
                    newdual_ref[k, block, cols] = (gain[:, cols] * moved).astype(jnp.bfloat16)
                    newz_ref[k, block, cols] = (
                        gap + target[k, block, cols].astype(jnp.float32) - blend[:, cols] * moved
                    ).astype(jnp.bfloat16)
                return carry

            lax.fori_loop(0, own_count * steps, tail, 0)

    for copy in started:
        copy.wait_send()


def step(tile_src, tile_count, request, feats, tiles, z_old, dual, target, w_rows, rho, beta, n_comm, n_wide):
    own_count, nodes, width = feats.shape
    slots = tiles.shape[1]
    hidden = w_rows.shape[1]
    gather_w = w_rows.shape[0] % 16 == 0
    if not gather_w:
        w_rows = lax.all_gather(w_rows, "wide", axis=0, tiled=True)
    cw = largest_block(width, 256, 128)
    chunks = width // cw
    column = largest_block(hidden, 256, 128)
    rows = largest_block(nodes, 384, 128)
    tail_rows = largest_block(nodes, 256, 128)
    plan = (chunks, cw, rows, tail_rows, column, gather_w)
    peers = n_comm - 1
    half = n_wide // 2
    bf16 = jnp.bfloat16
    smem = pl.BlockSpec(memory_space=pltpu.SMEM)
    vmem = pl.BlockSpec(memory_space=pltpu.VMEM)
    anywhere = pl.BlockSpec(memory_space=pl.ANY)
    dma = pltpu.SemaphoreType.DMA
    weight = pltpu.VMEM((n_wide,) + w_rows.shape if gather_w else w_rows.shape, bf16)
    return pl.pallas_call(
        functools.partial(step_kernel, n_comm, n_wide, plan),
        out_shape=[
            pltpu.VMEM(z_old.shape, bf16),
            pltpu.VMEM(dual.shape, bf16),
            pltpu.VMEM((width, own_count * nodes), bf16),
        ],
        in_specs=[smem] * 3 + [anywhere] * 6 + [vmem] * 2,
        out_specs=[vmem] * 3,
        scratch_shapes=[
            pltpu.VMEM(feats.shape, bf16),
            pltpu.VMEM(tiles.shape, bf16),
            pltpu.VMEM(z_old.shape, bf16),
            pltpu.VMEM(dual.shape, bf16),
            pltpu.VMEM(target.shape, bf16),
            weight,
            pltpu.VMEM(z_old.shape, jnp.float32),
            pltpu.VMEM((peers, 8, 128), jnp.int32),
            pltpu.VMEM((peers, 8, 128), jnp.int32),
        ]
        + [pltpu.VMEM((own_count + n_comm, nodes, cw), bf16)] * chunks
        + [pltpu.VMEM((peers, nodes, cw), bf16)] * chunks
        + [
            dma((1,)), dma((chunks,)), dma((1,)), dma((3,)), dma((1,)), dma((peers,)), dma((peers,)),
            dma((peers, chunks)), dma((peers, chunks)), dma((half,)), dma((half,)), dma((half,)), dma((half,)),
        ],
        compiler_params=pltpu.CompilerParams(
            collective_id=1, has_side_effects=True, vmem_limit_bytes=STEP_VMEM
        ),
        cost_estimate=pl.CostEstimate(flops=1 << 36, bytes_accessed=32 << 20, transcendentals=0),
    )(tile_src, tile_count, request, feats, tiles, z_old, dual, target, w_rows, rho, beta)


def reduce_kernel(
    n_comm, n_wide, factor, column, agg_ref, dual_ref, out_ref, grads, got_pair, sums, got_comm, parts, got_wide,
    final, pair_send, pair_recv, comm_send, comm_recv, wide_send, wide_recv, final_send, final_recv,
):
    half = n_wide // 2
    columns = sums.shape[-1]
    shard, hidden = out_ref.shape
    own_count, nodes, _ = dual_ref.shape
    c = lax.axis_index("comm")
    w = lax.axis_index("wide")
    mine = w // 2
    side = lax.rem(w, 2)
    partner = w + 1 - 2 * side

    def signal(to_c, to_w):
        pl.semaphore_signal(
            pltpu.get_barrier_semaphore(), inc=1, device_id=(to_c, to_w), device_id_type=MESH
        )

    signal(c, partner)
    for off in range(1, half):
        signal(c, lax.rem(mine + off, half) * 2 + side)
    for off in range(1, n_comm):
        signal(lax.rem(c + off, n_comm), w)

    def remote(src, dst, send, recv, to_c, to_w):
        return pltpu.make_async_remote_copy(
            src_ref=src, dst_ref=dst, send_sem=send, recv_sem=recv, device_id=(to_c, to_w),
            device_id_type=MESH,
        )

    def arrived(dst, recv):
        remote(dst, dst, recv, recv, c, partner).wait_recv()

    started = []

    def start(*args):
        copy = remote(*args)
        copy.start()
        started.append(copy)

    order = [lax.rem(mine + off, half) for off in range(1, half)] + [mine]

    def gradient(at, j):
        block = pl.ds(pl.multiple_of(j * (2 * shard), 2 * shard), 2 * shard)
        for n in range(hidden // column):
            cols = slice(n * column, (n + 1) * column)
            moved = dual_ref[:, :, cols].reshape(own_count * nodes, column)
            value = mxu(agg_ref[block, :], moved).astype(jnp.bfloat16)
            grads[at, 0, :, cols] = value[:shard]
            grads[at, 1, :, cols] = value[shard:]

    def combine(at):
        arrived(got_pair.at[at], pair_recv.at[at])
        value = grads[at, side].astype(jnp.float32) + got_pair[at].astype(jnp.float32)
        value = value.astype(jnp.bfloat16)
        for q in range(n_comm):
            sums[q, at] = value[:, q * columns : (q + 1) * columns]
        for off in (list(range(n_comm - 1, n_comm)) + list(range(1, n_comm - 1))):
            q = towards(off)
            start(
                sums.at[q, at], got_comm.at[c, at], comm_send.at[off - 1, at],
                comm_recv.at[c, at], q, w,
            )

    paired = n_comm & (n_comm - 1) == 0

    def towards(off):
        return lax.bitwise_xor(c, off) if paired else lax.rem(c + off, n_comm)

    for at, j in enumerate(order):
        gradient(at, j)
        if at == 0:
            pl.semaphore_wait(pltpu.get_barrier_semaphore(), 1 + (half - 1) + (n_comm - 1))
        start(
            grads.at[at, 1 - side], got_pair.at[at], pair_send.at[at], pair_recv.at[at], c, partner
        )
        if at > 0:
            combine(at - 1)
    combine(half - 1)
    for at, j in enumerate(order):
        value = sums[c, at].astype(jnp.float32)
        for off in range(1, n_comm):
            q = towards(off)
            arrived(got_comm.at[q, at], comm_recv.at[q, at])
            value = value + got_comm[q, at].astype(jnp.float32)
        if at < half - 1:
            parts[at] = value.astype(jnp.bfloat16)
            start(
                parts.at[at], got_wide.at[mine], wide_send.at[at], wide_recv.at[mine],
                c, j * 2 + side,
            )
        else:
            total = value
    for off in range(1, half):
        j = lax.rem(mine + off, half)
        arrived(got_wide.at[j], wide_recv.at[j])
        total = total + got_wide[j].astype(jnp.float32)
    final[c] = total.astype(jnp.bfloat16)
    for off in range(1, n_comm):
        start(final.at[c], final.at[c], final_send.at[off - 1], final_recv.at[c], towards(off), w)
    for off in range(1, n_comm):
        q = towards(off)
        arrived(final.at[q], final_recv.at[q])
    for q in range(n_comm):
        out_ref[:, q * columns : (q + 1) * columns] = final[q].astype(jnp.float32) * factor
    for copy in started:
        copy.wait_send()


def reduce_grad(agg_t, new_dual, n_comm, n_wide, factor):
    width = agg_t.shape[0]
    hidden = new_dual.shape[2]
    rows = width // n_wide
    half = n_wide // 2
    block = (rows, hidden)
    piece = (rows, hidden // n_comm)
    column = largest_block(hidden, 256, 128)
    return pl.pallas_call(
        functools.partial(reduce_kernel, n_comm, n_wide, factor, column),
        out_shape=pltpu.VMEM(block, jnp.float32),
        in_specs=[pl.BlockSpec(memory_space=pltpu.VMEM)] * 2,
        out_specs=pl.BlockSpec(memory_space=pltpu.VMEM),
        scratch_shapes=[
            pltpu.VMEM((half, 2) + block, jnp.bfloat16),
            pltpu.VMEM((half,) + block, jnp.bfloat16),
            pltpu.VMEM((n_comm, half) + piece, jnp.bfloat16),
            pltpu.VMEM((n_comm, half) + piece, jnp.bfloat16),
            pltpu.VMEM((half,) + piece, jnp.bfloat16),
            pltpu.VMEM((half,) + piece, jnp.bfloat16),
            pltpu.VMEM((n_comm,) + piece, jnp.bfloat16),
            pltpu.SemaphoreType.DMA((half,)),
            pltpu.SemaphoreType.DMA((half,)),
            pltpu.SemaphoreType.DMA((n_comm, half)),
            pltpu.SemaphoreType.DMA((n_comm, half)),
            pltpu.SemaphoreType.DMA((half,)),
            pltpu.SemaphoreType.DMA((half,)),
            pltpu.SemaphoreType.DMA((n_comm,)),
            pltpu.SemaphoreType.DMA((n_comm,)),
        ],
        compiler_params=pltpu.CompilerParams(
            collective_id=0, has_side_effects=True, vmem_limit_bytes=REDUCE_VMEM
        ),
        cost_estimate=pl.CostEstimate(flops=1 << 34, bytes_accessed=8 << 20, transcendentals=0),
    )(agg_t, new_dual)


def local(feats, tiles, tile_src, tile_count, request, z_old, dual, target, w_rows, rho, beta):
    own_count, nodes, _ = feats.shape
    hidden = w_rows.shape[1]
    n_comm = lax.axis_size("comm")
    n_wide = lax.axis_size("wide")
    new_z, new_dual, agg_t = step(
        tile_src, tile_count, request, feats, tiles, z_old, dual, target, w_rows,
        rho.reshape(1, hidden), beta.reshape(1, hidden), n_comm, n_wide,
    )
    factor = 1.0 / math.sqrt(own_count * nodes * n_comm * n_wide)
    return new_z, new_dual, reduce_grad(agg_t, new_dual, n_comm, n_wide, factor)


def solution(mesh):
    in_specs = (
        P(("comm", "wide"), None, None),
        P(("comm", "wide"), None, None, None),
        P(("comm", "wide"), None),
        P(("comm", "wide")),
        P(("comm", "wide"), None),
        P(("comm", "wide"), None, None),
        P(("comm", "wide"), None, None),
        P(("comm", "wide"), None, None),
        P("wide", None),
        P(),
        P(),
    )
    out_specs = (P(("comm", "wide"), None, None), P(("comm", "wide"), None, None), P("wide", None))
    return jax.shard_map(local, mesh=mesh, in_specs=in_specs, out_specs=out_specs, check_vma=False)
```

```python
import functools
import math

import jax
import jax.numpy as jnp
from jax import lax
from jax.experimental import pallas as pl
from jax.experimental.pallas import tpu as pltpu
from jax.sharding import PartitionSpec as P


STEP_VMEM = 40 * 1024 * 1024
FINISH_VMEM = 8 * 1024 * 1024
REDUCE_VMEM = 10 * 1024 * 1024

MESH = pl.DeviceIdType.MESH


def largest_block(size, limit, unit):
    for block in range(limit, 0, -unit):
        if size % block == 0:
            return block
    return size


def mxu(a, b):
    return jnp.dot(a, b, preferred_element_type=jnp.float32)


def pieces_of(nodes, width):
    cw = largest_block(width, 256, 128)
    last = largest_block(nodes, 256, 128)
    pieces = [(j * cw, 0, nodes) for j in range(width // cw - 1)]
    if last < nodes:
        pieces.append((width - cw, 0, nodes - last))
    pieces.append((width - cw, nodes - last if last < nodes else 0, last))
    return cw, pieces


def step_kernel(n_comm, n_wide, plan, *refs):
    (cw, pieces, rows, column, gather_w) = plan
    count = len(pieces)
    (src_hbm, count_hbm, request_hbm, feats_ref, tiles_ref, z_ref, dual_ref, target_ref, w_ref, rho_ref,
     beta_ref, part, agg_t, agg_last, w_last, z_old, target, coef, src_ref, count_ref, request_ref, rates,
     own, tiles, dual, weight, held, ask, asked) = refs[:29]
    pools = refs[29 : 29 + count]
    stages = refs[29 + count : 29 + 2 * count]
    (small_sem, own_sem, pool_sem, tile_sem, data_sem, w_sem, ask_send, ask_recv, feat_send, feat_recv,
     w_send, w_recv, fwd_send, fwd_recv) = refs[29 + 2 * count :]
    own_count, nodes, width = feats_ref.shape
    slots = tiles_ref.shape[1]
    hidden = w_ref.shape[-1]
    peers = n_comm - 1
    paired = n_comm & (n_comm - 1) == 0
    half = n_wide // 2
    dead = own_count + peers
    c = lax.axis_index("comm")
    w = lax.axis_index("wide")
    chip = w // 2
    side = lax.rem(w, 2)
    partner = w + 1 - 2 * side

    def towards(off):
        return lax.bitwise_xor(c, off) if paired else lax.rem(c + off, n_comm)

    def arriving(off):
        return lax.bitwise_xor(c, off) if paired else lax.rem(c - off + n_comm, n_comm)

    def along(off):
        return lax.rem(chip + off, half) * 2 + side

    def signal(to_c, to_w):
        pl.semaphore_signal(
            pltpu.get_barrier_semaphore(), inc=1, device_id=(to_c, to_w), device_id_type=MESH
        )

    def remote(src, dst, send, recv, to_c, to_w):
        return pltpu.make_async_remote_copy(
            src_ref=src, dst_ref=dst, send_sem=send, recv_sem=recv, device_id=(to_c, to_w),
            device_id_type=MESH,
        )

    def arrived(dst, recv):
        remote(dst, dst, recv, recv, c, partner).wait_recv()

    request_copy = pltpu.make_async_copy(request_hbm, request_ref, small_sem.at[0])
    request_copy.start()
    for off in range(1, n_comm):
        signal(lax.rem(c + off, n_comm), w)
    greeted = peers
    if gather_w:
        for off in range(1, half):
            signal(c, along(off))
        signal(c, partner)
        greeted += half
    own_copy = pltpu.make_async_copy(feats_ref, own, own_sem.at[0])
    own_copy.start()
    w_copy = pltpu.make_async_copy(w_ref, weight.at[w] if gather_w else weight, w_sem.at[0])
    w_copy.start()
    small_copies = [
        pltpu.make_async_copy(src_hbm, src_ref, small_sem.at[1]),
        pltpu.make_async_copy(count_hbm, count_ref, small_sem.at[2]),
        pltpu.make_async_copy(rho_ref, rates.at[0], small_sem.at[3]),
        pltpu.make_async_copy(beta_ref, rates.at[1], small_sem.at[4]),
    ]
    pool_copies = [
        pltpu.make_async_copy(
            feats_ref.at[:, pl.ds(row, size), pl.ds(col, cw)], pools[p].at[pl.ds(0, own_count)], pool_sem.at[p]
        )
        for p, (col, row, size) in enumerate(pieces)
    ]
    tile_copy = pltpu.make_async_copy(tiles_ref, tiles, tile_sem.at[0])
    data_copies = [
        pltpu.make_async_copy(dual_ref, dual, data_sem.at[0]),
        pltpu.make_async_copy(target_ref, target, data_sem.at[1]),
        pltpu.make_async_copy(z_ref, z_old, data_sem.at[2]),
    ]
    request_copy.wait()
    for off in range(1, n_comm):
        ask[off - 1] = jnp.full(ask.shape[1:], request_ref[0, arriving(off)], jnp.int32)
    pl.semaphore_wait(pltpu.get_barrier_semaphore(), greeted)

    started = []

    def start(*args):
        copy = remote(*args)
        copy.start()
        started.append(copy)

    near = list(range(1, peers)) + [peers]
    far = [peers] + list(range(1, peers))
    for off in far:
        start(ask.at[off - 1], asked.at[off - 1], ask_send.at[off - 1], ask_recv.at[off - 1], arriving(off), w)
    for copy in small_copies + pool_copies + [tile_copy] + data_copies:
        copy.start()
    own_copy.wait()
    wants = {}
    for p, (col, row, size) in enumerate(pieces):
        for off in near if p == 0 else far:
            if p == 0:
                arrived(asked.at[off - 1], ask_recv.at[off - 1])
                wants[off] = jnp.clip(jnp.max(asked[off - 1]), 0, own_count - 1)
            stages[p][off - 1] = own[wants[off], row : row + size, col : col + cw]
            start(
                stages[p].at[off - 1], pools[p].at[own_count + off - 1], feat_send.at[off - 1, p],
                feat_recv.at[off - 1, p], towards(off), w,
            )
    w_copy.wait()
    if gather_w:
        for off in range(1, half):
            start(weight.at[w], weight.at[w], w_send.at[off - 1], w_recv.at[chip], c, along(off))
        start(weight.at[w], weight.at[w], fwd_send.at[0], fwd_recv.at[chip], c, partner)
    for p, (col, row, size) in enumerate(pieces):
        pools[p][dead] = jnp.zeros((size, cw), jnp.bfloat16)
    for copy in small_copies:
        copy.wait()

    def pick(k, t):
        source = src_ref[k, t]
        member = jnp.maximum(source - own_count, 0)
        if paired:
            offset = lax.bitwise_xor(c, member)
        else:
            offset = lax.rem(c - member + n_comm, n_comm)
        other = jnp.where(member == c, request_ref[0, c], own_count + offset - 1)
        index = jnp.where(source < own_count, source, other)
        index = jnp.clip(index, 0, dead - 1)
        return jnp.where(t < count_ref[k], index, dead)

    rho = rates[0]
    beta = rates[1]
    inverse = 1.0 / rho
    blend = beta / (rho + beta)
    coef[0:1] = blend
    coef[1:2] = rho * blend

    def products(p, k, block):
        (_, row, size) = pieces[p]
        total = mxu(tiles[k, 0, block, row : row + size], pools[p][pick(k, 0)])
        for t in range(1, slots):
            total = total + mxu(tiles[k, t, block, row : row + size], pools[p][pick(k, t)])
        return total

    if gather_w:
        for off in range(1, half):
            other = along(off)
            arrived(weight.at[other], w_recv.at[other // 2])
            start(weight.at[other], weight.at[other], fwd_send.at[off], fwd_recv.at[other // 2], c, partner)
        for at in range(half):
            arrived(weight.at[at * 2 + 1 - side], fwd_recv.at[at])
    tile_copy.wait()
    for copy in data_copies:
        copy.wait()

    def w_rows_of(col, cols):
        if gather_w:
            return weight[...].reshape(width, hidden)[col : col + cw, cols]
        return weight[col : col + cw, cols]

    for at in range(hidden // column):
        cols = slice(at * column, (at + 1) * column)
        w_last[:, cols] = w_rows_of(width - cw, cols)

    for p, (col, row, size) in enumerate(pieces):
        pool_copies[p].wait()
        for off in far:
            arrived(pools[p].at[own_count + off - 1], feat_recv.at[off - 1, p])
        if p == count - 1:
            for k in range(own_count):
                for step in range(nodes // rows):
                    block = slice(step * rows, (step + 1) * rows)
                    total = products(p, k, block)
                    if count > width // cw:
                        total = total + held[k, block]
                    agg = total.astype(jnp.bfloat16)
                    agg_last[k, block] = agg
                    at = k * nodes + step * rows
                    agg_t[col : col + cw, at : at + rows] = agg.T
            continue
        steps = nodes // rows

        def body(step, carry, p=p, col=col, steps=steps):
            k = step // steps
            at = lax.rem(step, steps)
            block = pl.ds(pl.multiple_of(at * rows, rows), rows)
            total = products(p, k, block)
            if col == width - cw:
                held[k, block] = total
                return carry
            agg = total.astype(jnp.bfloat16)
            agg_t[col : col + cw, pl.ds(pl.multiple_of(k * nodes + at * rows, 128), rows)] = agg.T
            for n in range(hidden // column):
                cols = slice(n * column, (n + 1) * column)
                value = mxu(agg, w_rows_of(col, cols))
                if p == 0:
                    value = value + (
                        dual[k, block, cols].astype(jnp.float32) * inverse[:, cols]
                        - target[k, block, cols].astype(jnp.float32)
                    )
                else:
                    value = value + part[k, block, cols]
                part[k, block, cols] = value
            return carry

        lax.fori_loop(0, own_count * steps, body, 0)
    for copy in started:
        copy.wait_send()


def step(tile_src, tile_count, request, feats, tiles, z_old, dual, target, w_rows, rho, beta, n_comm, n_wide):
    own_count, nodes, width = feats.shape
    hidden = w_rows.shape[1]
    gather_w = w_rows.shape[0] % 16 == 0
    if not gather_w:
        w_rows = lax.all_gather(w_rows, "wide", axis=0, tiled=True)
    cw, pieces = pieces_of(nodes, width)
    column = largest_block(hidden, 256, 128)
    rows = largest_block(nodes, 384, 128)
    plan = (cw, pieces, rows, column, gather_w)
    peers = n_comm - 1
    half = n_wide // 2
    count = len(pieces)
    bf16 = jnp.bfloat16
    f32 = jnp.float32
    dma = pltpu.SemaphoreType.DMA
    weight = pltpu.VMEM((n_wide,) + w_rows.shape if gather_w else w_rows.shape, bf16)
    return pl.pallas_call(
        functools.partial(step_kernel, n_comm, n_wide, plan),
        out_shape=[
            pltpu.VMEM(z_old.shape, f32),
            pltpu.VMEM((width, own_count * nodes), bf16),
            pltpu.VMEM((own_count, nodes, cw), bf16),
            pltpu.VMEM((cw, hidden), bf16),
            pltpu.VMEM(z_old.shape, bf16),
            pltpu.VMEM(target.shape, bf16),
            pltpu.VMEM((2, hidden), f32),
        ],
        in_specs=[pl.BlockSpec(memory_space=pl.ANY)] * 11,
        out_specs=[pl.BlockSpec(memory_space=pltpu.VMEM)] * 7,
        scratch_shapes=[
            pltpu.SMEM(tile_src.shape, jnp.int32),
            pltpu.SMEM(tile_count.shape, jnp.int32),
            pltpu.SMEM(request.shape, jnp.int32),
            pltpu.VMEM((2, 1, hidden), f32),
            pltpu.VMEM(feats.shape, bf16),
            pltpu.VMEM(tiles.shape, bf16),
            pltpu.VMEM(dual.shape, bf16),
            weight,
            pltpu.VMEM((own_count, nodes, cw), f32),
            pltpu.VMEM((peers, 8, 128), jnp.int32),
            pltpu.VMEM((peers, 8, 128), jnp.int32),
        ]
        + [pltpu.VMEM((own_count + n_comm, size, cw), bf16) for (_, _, size) in pieces]
        + [pltpu.VMEM((peers, size, cw), bf16) for (_, _, size) in pieces]
        + [
            dma((5,)), dma((1,)), dma((count,)), dma((1,)), dma((3,)), dma((1,)), dma((peers,)), dma((peers,)),
            dma((peers, count)), dma((peers, count)), dma((half,)), dma((half,)), dma((half,)), dma((half,)),
        ],
        compiler_params=pltpu.CompilerParams(
            collective_id=1, has_side_effects=True, vmem_limit_bytes=STEP_VMEM
        ),
        cost_estimate=pl.CostEstimate(flops=1 << 36, bytes_accessed=32 << 20, transcendentals=0),
    )(tile_src, tile_count, request, feats, tiles, z_old, dual, target, w_rows, rho, beta)


def finish_kernel(
    n_wide, rows, column, part, agg_t, agg_last, w_last, z_old, target, coef, newz_ref, newdual_ref, moved_ref,
    grads, newz, sems,
):
    own_count, nodes, hidden = part.shape
    _, shard, _ = grads.shape
    half = n_wide // 2
    j = lax.rem(lax.axis_index("wide") // 2 + 1, half)
    blend = coef[0:1]
    gain = coef[1:2]
    copies = []
    for k in range(own_count):
        for step in range(nodes // rows):
            block = slice(step * rows, (step + 1) * rows)
            agg = agg_last[k, block]
            for n in range(hidden // column):
                cols = slice(n * column, (n + 1) * column)
                gap = mxu(agg, w_last[:, cols]) + part[k, block, cols]
                moved = jnp.where(z_old[k, block, cols].astype(jnp.float32) > 0, gap, 0.0)
                moved_ref[k, block, cols] = (gain[:, cols] * moved).astype(jnp.bfloat16)
                newz[k, block, cols] = (
                    gap + target[k, block, cols].astype(jnp.float32) - blend[:, cols] * moved
                ).astype(jnp.bfloat16)
            for src, dst in ((newz, newz_ref), (moved_ref, newdual_ref)):
                copy = pltpu.make_async_copy(src.at[k, block], dst.at[k, block], sems.at[len(copies)])
                copy.start()
                copies.append(copy)
    gradient(agg_t, moved_ref, grads, j, column)
    for copy in copies:
        copy.wait()


def gradient(agg_t, moved_ref, grads, j, column):
    own_count, nodes, hidden = moved_ref.shape
    _, shard, _ = grads.shape
    block = pl.ds(pl.multiple_of(j * (2 * shard), 2 * shard), 2 * shard)
    for n in range(hidden // column):
        cols = slice(n * column, (n + 1) * column)
        moved = moved_ref[:, :, cols].reshape(own_count * nodes, column)
        value = mxu(agg_t[block, :], moved).astype(jnp.bfloat16)
        grads[0, :, cols] = value[:shard]
        grads[1, :, cols] = value[shard:]


def finish(part, agg_t, agg_last, w_last, z_old, target, coef, n_wide):
    own_count, nodes, hidden = part.shape
    width = agg_t.shape[0]
    rows = largest_block(nodes, 256, 128)
    column = largest_block(hidden, 256, 128)
    vmem = pl.BlockSpec(memory_space=pltpu.VMEM)
    anywhere = pl.BlockSpec(memory_space=pl.ANY)
    bf16 = jnp.bfloat16
    return pl.pallas_call(
        functools.partial(finish_kernel, n_wide, rows, column),
        out_shape=[
            jax.ShapeDtypeStruct(part.shape, bf16),
            jax.ShapeDtypeStruct(part.shape, bf16),
            pltpu.VMEM(part.shape, bf16),
            pltpu.VMEM((2, width // n_wide, hidden), bf16),
        ],
        in_specs=[vmem] * 7,
        out_specs=[pl.BlockSpec(memory_space=pltpu.HBM)] * 2 + [vmem] * 2,
        scratch_shapes=[
            pltpu.VMEM(part.shape, bf16),
            pltpu.SemaphoreType.DMA((2 * own_count * (nodes // rows),)),
        ],
        compiler_params=pltpu.CompilerParams(vmem_limit_bytes=FINISH_VMEM),
        cost_estimate=pl.CostEstimate(flops=1 << 32, bytes_accessed=8 << 20, transcendentals=0),
    )(part, agg_t, agg_last, w_last, z_old, target, coef)


def reduce_kernel(
    n_comm, n_wide, factor, column, agg_ref, dual_ref, first_ref, out_ref, grads, got_pair, sums, got_comm, parts, got_wide,
    final, pair_send, pair_recv, comm_send, comm_recv, wide_send, wide_recv, final_send, final_recv,
):
    half = n_wide // 2
    columns = sums.shape[-1]
    shard, hidden = out_ref.shape
    own_count, nodes, _ = dual_ref.shape
    c = lax.axis_index("comm")
    w = lax.axis_index("wide")
    mine = w // 2
    side = lax.rem(w, 2)
    partner = w + 1 - 2 * side

    def signal(to_c, to_w):
        pl.semaphore_signal(
            pltpu.get_barrier_semaphore(), inc=1, device_id=(to_c, to_w), device_id_type=MESH
        )

    signal(c, partner)
    for off in range(1, half):
        signal(c, lax.rem(mine + off, half) * 2 + side)
    for off in range(1, n_comm):
        signal(lax.rem(c + off, n_comm), w)

    def remote(src, dst, send, recv, to_c, to_w):
        return pltpu.make_async_remote_copy(
            src_ref=src, dst_ref=dst, send_sem=send, recv_sem=recv, device_id=(to_c, to_w),
            device_id_type=MESH,
        )

    def arrived(dst, recv):
        remote(dst, dst, recv, recv, c, partner).wait_recv()

    started = []

    def start(*args):
        copy = remote(*args)
        copy.start()
        started.append(copy)

    order = [lax.rem(mine + off, half) for off in range(1, half)] + [mine]

    def partial(at):
        return first_ref if at == 0 else grads.at[at - 1]

    def combine(at):
        arrived(got_pair.at[at], pair_recv.at[at])
        value = partial(at)[side].astype(jnp.float32) + got_pair[at].astype(jnp.float32)
        value = value.astype(jnp.bfloat16)
        for q in range(n_comm):
            sums[q, at] = value[:, q * columns : (q + 1) * columns]
        for off in (list(range(n_comm - 1, n_comm)) + list(range(1, n_comm - 1))):
            q = towards(off)
            start(
                sums.at[q, at], got_comm.at[c, at], comm_send.at[off - 1, at],
                comm_recv.at[c, at], q, w,
            )

    paired = n_comm & (n_comm - 1) == 0

    def towards(off):
        return lax.bitwise_xor(c, off) if paired else lax.rem(c + off, n_comm)

    for at, j in enumerate(order):
        if at > 0:
            gradient(agg_ref, dual_ref, grads.at[at - 1], j, column)
        if at == 0:
            pl.semaphore_wait(pltpu.get_barrier_semaphore(), 1 + (half - 1) + (n_comm - 1))
        start(
            partial(at).at[1 - side], got_pair.at[at], pair_send.at[at], pair_recv.at[at], c, partner
        )
        if at > 0:
            combine(at - 1)
    combine(half - 1)
    for at, j in enumerate(order):
        value = sums[c, at].astype(jnp.float32)
        for off in range(1, n_comm):
            q = towards(off)
            arrived(got_comm.at[q, at], comm_recv.at[q, at])
            value = value + got_comm[q, at].astype(jnp.float32)
        if at < half - 1:
            parts[at] = value.astype(jnp.bfloat16)
            start(
                parts.at[at], got_wide.at[mine], wide_send.at[at], wide_recv.at[mine],
                c, j * 2 + side,
            )
        else:
            total = value
    for off in range(1, half):
        j = lax.rem(mine + off, half)
        arrived(got_wide.at[j], wide_recv.at[j])
        total = total + got_wide[j].astype(jnp.float32)
    final[c] = total.astype(jnp.bfloat16)
    for off in range(1, n_comm):
        start(final.at[c], final.at[c], final_send.at[off - 1], final_recv.at[c], towards(off), w)
    for off in range(1, n_comm):
        q = towards(off)
        arrived(final.at[q], final_recv.at[q])
    for q in range(n_comm):
        out_ref[:, q * columns : (q + 1) * columns] = final[q].astype(jnp.float32) * factor
    for copy in started:
        copy.wait_send()


def reduce_grad(agg_t, new_dual, first, n_comm, n_wide, factor):
    width = agg_t.shape[0]
    hidden = new_dual.shape[2]
    rows = width // n_wide
    half = n_wide // 2
    block = (rows, hidden)
    piece = (rows, hidden // n_comm)
    column = largest_block(hidden, 256, 128)
    return pl.pallas_call(
        functools.partial(reduce_kernel, n_comm, n_wide, factor, column),
        out_shape=pltpu.VMEM(block, jnp.float32),
        in_specs=[pl.BlockSpec(memory_space=pltpu.VMEM)] * 3,
        out_specs=pl.BlockSpec(memory_space=pltpu.VMEM),
        scratch_shapes=[
            pltpu.VMEM((half - 1, 2) + block, jnp.bfloat16),
            pltpu.VMEM((half,) + block, jnp.bfloat16),
            pltpu.VMEM((n_comm, half) + piece, jnp.bfloat16),
            pltpu.VMEM((n_comm, half) + piece, jnp.bfloat16),
            pltpu.VMEM((half,) + piece, jnp.bfloat16),
            pltpu.VMEM((half,) + piece, jnp.bfloat16),
            pltpu.VMEM((n_comm,) + piece, jnp.bfloat16),
            pltpu.SemaphoreType.DMA((half,)),
            pltpu.SemaphoreType.DMA((half,)),
            pltpu.SemaphoreType.DMA((n_comm, half)),
            pltpu.SemaphoreType.DMA((n_comm, half)),
            pltpu.SemaphoreType.DMA((half,)),
            pltpu.SemaphoreType.DMA((half,)),
            pltpu.SemaphoreType.DMA((n_comm,)),
            pltpu.SemaphoreType.DMA((n_comm,)),
        ],
        compiler_params=pltpu.CompilerParams(
            collective_id=0, has_side_effects=True, vmem_limit_bytes=REDUCE_VMEM
        ),
        cost_estimate=pl.CostEstimate(flops=1 << 34, bytes_accessed=8 << 20, transcendentals=0),
    )(agg_t, new_dual, first)


def local(feats, tiles, tile_src, tile_count, request, z_old, dual, target, w_rows, rho, beta):
    own_count, nodes, _ = feats.shape
    hidden = w_rows.shape[1]
    n_comm = lax.axis_size("comm")
    n_wide = lax.axis_size("wide")
    part, agg_t, agg_last, w_last, z_old, target, coef = step(
        tile_src, tile_count, request, feats, tiles, z_old, dual, target, w_rows,
        rho.reshape(1, hidden), beta.reshape(1, hidden), n_comm, n_wide,
    )
    new_z, new_dual, moved, first = finish(part, agg_t, agg_last, w_last, z_old, target, coef, n_wide)
    factor = 1.0 / math.sqrt(own_count * nodes * n_comm * n_wide)
    return new_z, new_dual, reduce_grad(agg_t, moved, first, n_comm, n_wide, factor)


def solution(mesh):
    in_specs = (
        P(("comm", "wide"), None, None),
        P(("comm", "wide"), None, None, None),
        P(("comm", "wide"), None),
        P(("comm", "wide")),
        P(("comm", "wide"), None),
        P(("comm", "wide"), None, None),
        P(("comm", "wide"), None, None),
        P(("comm", "wide"), None, None),
        P("wide", None),
        P(),
        P(),
    )
    out_specs = (P(("comm", "wide"), None, None), P(("comm", "wide"), None, None), P("wide", None))
    return jax.shard_map(local, mesh=mesh, in_specs=in_specs, out_specs=out_specs, check_vma=False)
```

```python
import functools
import math

import jax
import jax.numpy as jnp
from jax import lax
from jax.experimental import pallas as pl
from jax.experimental.pallas import tpu as pltpu
from jax.sharding import PartitionSpec as P


STEP_VMEM = 40 * 1024 * 1024
FINISH_VMEM = 8 * 1024 * 1024
REDUCE_VMEM = 10 * 1024 * 1024

MESH = pl.DeviceIdType.MESH


def largest_block(size, limit, unit):
    for block in range(limit, 0, -unit):
        if size % block == 0:
            return block
    return size


def mxu(a, b):
    return jnp.dot(a, b, preferred_element_type=jnp.float32)


def pieces_of(nodes, width):
    cw = largest_block(width, 256, 128)
    last = largest_block(nodes, 256, 128)
    early = 128 if cw == 256 and nodes > 128 and width > 2 * cw else 0
    pieces = [(0, early, early, nodes - early), (early, cw - early, 0, nodes)] if early else [(0, cw, 0, nodes)]
    pieces += [(j * cw, cw, 0, nodes) for j in range(1, width // cw - 1)]
    if last < nodes:
        pieces.append((width - cw, cw, 0, nodes - last))
    pieces.append((width - cw, cw, nodes - last if last < nodes else 0, last))
    return cw, early, pieces


def step_kernel(n_comm, n_wide, plan, *refs):
    (cw, early, pieces, rows, column, gather_w) = plan
    count = len(pieces)
    (src_hbm, count_hbm, request_hbm, feats_ref, tiles_ref, z_ref, dual_ref, target_ref, w_ref, rho_ref,
     beta_ref, part, agg_t, agg_last, w_last, scale, target, coef, src_ref, count_ref, request_ref, rates,
     own, tiles, dual, z_old, weight, held, ask, asked, eager) = refs[:31]
    pools = refs[31 : 31 + count]
    stages = refs[31 + count : 31 + 2 * count]
    (small_sem, own_sem, pool_sem, tile_sem, data_sem, w_sem, ask_send, ask_recv, feat_send, feat_recv,
     w_send, w_recv, fwd_send, fwd_recv, eager_sem, eager_send, eager_recv) = refs[31 + 2 * count :]
    own_count, nodes, width = feats_ref.shape
    slots = tiles_ref.shape[1]
    hidden = w_ref.shape[-1]
    peers = n_comm - 1
    paired = n_comm & (n_comm - 1) == 0
    half = n_wide // 2
    dead = own_count + peers
    c = lax.axis_index("comm")
    w = lax.axis_index("wide")
    chip = w // 2
    side = lax.rem(w, 2)
    partner = w + 1 - 2 * side

    def towards(off):
        return lax.bitwise_xor(c, off) if paired else lax.rem(c + off, n_comm)

    def arriving(off):
        return lax.bitwise_xor(c, off) if paired else lax.rem(c - off + n_comm, n_comm)

    def along(off):
        return lax.rem(chip + off, half) * 2 + side

    def signal(to_c, to_w):
        pl.semaphore_signal(
            pltpu.get_barrier_semaphore(), inc=1, device_id=(to_c, to_w), device_id_type=MESH
        )

    def remote(src, dst, send, recv, to_c, to_w):
        return pltpu.make_async_remote_copy(
            src_ref=src, dst_ref=dst, send_sem=send, recv_sem=recv, device_id=(to_c, to_w),
            device_id_type=MESH,
        )

    def arrived(dst, recv):
        remote(dst, dst, recv, recv, c, partner).wait_recv()

    request_copy = pltpu.make_async_copy(request_hbm, request_ref, small_sem.at[0])
    request_copy.start()
    for off in range(1, n_comm):
        signal(lax.rem(c + off, n_comm), w)
    greeted = peers
    if gather_w:
        for off in range(1, half):
            signal(c, along(off))
        signal(c, partner)
        greeted += half
    eager_copy = None
    if early:
        eager_copy = pltpu.make_async_copy(
            feats_ref.at[:, pl.ds(0, early), pl.ds(0, early)], eager.at[pl.ds(0, own_count)], eager_sem.at[0]
        )
        eager_copy.start()
    own_copy = pltpu.make_async_copy(feats_ref, own, own_sem.at[0])
    own_copy.start()
    w_copy = pltpu.make_async_copy(w_ref, weight.at[w] if gather_w else weight, w_sem.at[0])
    w_copy.start()
    small_copies = [
        pltpu.make_async_copy(src_hbm, src_ref, small_sem.at[1]),
        pltpu.make_async_copy(count_hbm, count_ref, small_sem.at[2]),
        pltpu.make_async_copy(rho_ref, rates.at[0], small_sem.at[3]),
        pltpu.make_async_copy(beta_ref, rates.at[1], small_sem.at[4]),
    ]
    pool_copies = [
        pltpu.make_async_copy(
            feats_ref.at[:, pl.ds(row, size), pl.ds(col, wide)], pools[p].at[pl.ds(0, own_count)], pool_sem.at[p]
        )
        for p, (col, wide, row, size) in enumerate(pieces)
    ]
    tile_copy = pltpu.make_async_copy(tiles_ref, tiles, tile_sem.at[0])
    data_copies = [
        pltpu.make_async_copy(dual_ref, dual, data_sem.at[0]),
        pltpu.make_async_copy(target_ref, target, data_sem.at[1]),
        pltpu.make_async_copy(z_ref, z_old, data_sem.at[2]),
    ]
    request_copy.wait()
    for off in range(1, n_comm):
        ask[off - 1] = jnp.full(ask.shape[1:], request_ref[0, arriving(off)], jnp.int32)
    pl.semaphore_wait(pltpu.get_barrier_semaphore(), greeted)

    started = []

    def start(*args):
        copy = remote(*args)
        copy.start()
        started.append(copy)

    near = list(range(1, peers)) + [peers]
    far = [peers] + list(range(1, peers))
    for off in far:
        start(ask.at[off - 1], asked.at[off - 1], ask_send.at[off - 1], ask_recv.at[off - 1], arriving(off), w)
    if early:
        eager_copy.wait()
        for off in far:
            start(
                eager.at[pl.ds(0, own_count)], eager.at[pl.ds(own_count * off, own_count)],
                eager_send.at[off - 1], eager_recv.at[off - 1], towards(off), w,
            )
    for copy in small_copies + pool_copies + [tile_copy] + data_copies:
        copy.start()
    own_copy.wait()
    wants = {}
    for p, (col, wide, row, size) in enumerate(pieces):
        for off in near if p == 0 else far:
            if p == 0:
                arrived(asked.at[off - 1], ask_recv.at[off - 1])
                wants[off] = jnp.clip(jnp.max(asked[off - 1]), 0, own_count - 1)
            stages[p][off - 1] = own[wants[off], row : row + size, col : col + wide]
            start(
                stages[p].at[off - 1], pools[p].at[own_count + off - 1], feat_send.at[off - 1, p],
                feat_recv.at[off - 1, p], towards(off), w,
            )
    w_copy.wait()
    if gather_w:
        for off in range(1, half):
            start(weight.at[w], weight.at[w], w_send.at[off - 1], w_recv.at[chip], c, along(off))
        start(weight.at[w], weight.at[w], fwd_send.at[0], fwd_recv.at[chip], c, partner)
    for p, (_, wide, _, size) in enumerate(pieces):
        pools[p][dead] = jnp.zeros((size, wide), jnp.bfloat16)
    if early:
        eager[own_count * n_comm] = jnp.zeros((early, early), jnp.bfloat16)
    for copy in small_copies:
        copy.wait()

    def pick(k, t):
        source = src_ref[k, t]
        member = jnp.maximum(source - own_count, 0)
        if paired:
            offset = lax.bitwise_xor(c, member)
        else:
            offset = lax.rem(c - member + n_comm, n_comm)
        other = jnp.where(member == c, request_ref[0, c], own_count + offset - 1)
        index = jnp.where(source < own_count, source, other)
        index = jnp.clip(index, 0, dead - 1)
        return jnp.where(t < count_ref[k], index, dead)

    def pick_eager(k, t):
        source = src_ref[k, t]
        member = jnp.clip(source - own_count, 0, peers)
        if paired:
            offset = lax.bitwise_xor(c, member)
        else:
            offset = lax.rem(c - member + n_comm, n_comm)
        index = jnp.where(source < own_count, source, own_count * offset + request_ref[0, member])
        index = jnp.clip(index, 0, own_count * n_comm - 1)
        return jnp.where(t < count_ref[k], index, own_count * n_comm)

    rho = rates[0]
    beta = rates[1]
    inverse = 1.0 / rho
    blend = beta / (rho + beta)
    gain = rho * blend
    coef[0:1] = inverse

    def products(p, k, block):
        (_, _, row, size) = pieces[p]
        total = mxu(tiles[k, 0, block, row : row + size], pools[p][pick(k, 0)])
        for t in range(1, slots):
            total = total + mxu(tiles[k, t, block, row : row + size], pools[p][pick(k, t)])
        if early and p == 0:
            for t in range(slots):
                total = total + mxu(tiles[k, t, block, :early], eager[pick_eager(k, t)])
        return total

    if gather_w:
        for off in range(1, half):
            other = along(off)
            arrived(weight.at[other], w_recv.at[other // 2])
            start(weight.at[other], weight.at[other], fwd_send.at[off], fwd_recv.at[other // 2], c, partner)
        for at in range(half):
            arrived(weight.at[at * 2 + 1 - side], fwd_recv.at[at])
    tile_copy.wait()
    for copy in data_copies:
        copy.wait()

    def w_rows_of(col, wide, cols):
        if gather_w:
            return weight[...].reshape(width, hidden)[col : col + wide, cols]
        return weight[col : col + wide, cols]

    for at in range(hidden // column):
        cols = slice(at * column, (at + 1) * column)
        w_last[:, cols] = w_rows_of(width - cw, cw, cols)

    for p, (col, wide, row, size) in enumerate(pieces):
        pool_copies[p].wait()
        if early and p == 0:
            for off in far:
                arrived(eager.at[pl.ds(own_count * off, own_count)], eager_recv.at[off - 1])
        for off in far:
            arrived(pools[p].at[own_count + off - 1], feat_recv.at[off - 1, p])
        if p == count - 1:
            for k in range(own_count):
                for step in range(nodes // rows):
                    block = slice(step * rows, (step + 1) * rows)
                    total = products(p, k, block)
                    if size < nodes:
                        total = total + held[k, block]
                    agg = total.astype(jnp.bfloat16)
                    agg_last[k, block] = agg
                    at = k * nodes + step * rows
                    agg_t[col : col + cw, at : at + rows] = agg.T
            continue
        steps = nodes // rows

        def body(step, carry, p=p, col=col, wide=wide, steps=steps):
            k = step // steps
            at = lax.rem(step, steps)
            block = pl.ds(pl.multiple_of(at * rows, rows), rows)
            total = products(p, k, block)
            if col == width - cw:
                held[k, block] = total
                return carry
            if p == 0:
                for n in range(hidden // column):
                    cols = slice(n * column, (n + 1) * column)
                    active = z_old[k, block, cols].astype(jnp.float32) > 0
                    scale[k, block, cols] = jnp.where(active, jnp.broadcast_to(gain[:, cols], active.shape), 0.0)
            agg = total.astype(jnp.bfloat16)
            agg_t[col : col + wide, pl.ds(pl.multiple_of(k * nodes + at * rows, 128), rows)] = agg.T
            for n in range(hidden // column):
                cols = slice(n * column, (n + 1) * column)
                value = mxu(agg, w_rows_of(col, wide, cols))
                if p == 0:
                    value = value + (
                        dual[k, block, cols].astype(jnp.float32) * inverse[:, cols]
                        - target[k, block, cols].astype(jnp.float32)
                    )
                else:
                    value = value + part[k, block, cols]
                part[k, block, cols] = value
            return carry

        lax.fori_loop(0, own_count * steps, body, 0)
    for copy in started:
        copy.wait_send()


def step(tile_src, tile_count, request, feats, tiles, z_old, dual, target, w_rows, rho, beta, n_comm, n_wide):
    own_count, nodes, width = feats.shape
    hidden = w_rows.shape[1]
    gather_w = w_rows.shape[0] % 16 == 0
    if not gather_w:
        w_rows = lax.all_gather(w_rows, "wide", axis=0, tiled=True)
    cw, early, pieces = pieces_of(nodes, width)
    column = largest_block(hidden, 256, 128)
    rows = largest_block(nodes, 384, 128)
    plan = (cw, early, pieces, rows, column, gather_w)
    peers = n_comm - 1
    half = n_wide // 2
    count = len(pieces)
    bf16 = jnp.bfloat16
    f32 = jnp.float32
    dma = pltpu.SemaphoreType.DMA
    weight = pltpu.VMEM((n_wide,) + w_rows.shape if gather_w else w_rows.shape, bf16)
    return pl.pallas_call(
        functools.partial(step_kernel, n_comm, n_wide, plan),
        out_shape=[
            pltpu.VMEM(z_old.shape, f32),
            pltpu.VMEM((width, own_count * nodes), bf16),
            pltpu.VMEM((own_count, nodes, cw), bf16),
            pltpu.VMEM((cw, hidden), bf16),
            pltpu.VMEM(z_old.shape, f32),
            pltpu.VMEM(target.shape, bf16),
            pltpu.VMEM((1, hidden), f32),
        ],
        in_specs=[pl.BlockSpec(memory_space=pl.ANY)] * 11,
        out_specs=[pl.BlockSpec(memory_space=pltpu.VMEM)] * 7,
        scratch_shapes=[
            pltpu.SMEM(tile_src.shape, jnp.int32),
            pltpu.SMEM(tile_count.shape, jnp.int32),
            pltpu.SMEM(request.shape, jnp.int32),
            pltpu.VMEM((2, 1, hidden), f32),
            pltpu.VMEM(feats.shape, bf16),
            pltpu.VMEM(tiles.shape, bf16),
            pltpu.VMEM(dual.shape, bf16),
            pltpu.VMEM(z_old.shape, bf16),
            weight,
            pltpu.VMEM((own_count, nodes, cw), f32),
            pltpu.VMEM((peers, 8, 128), jnp.int32),
            pltpu.VMEM((peers, 8, 128), jnp.int32),
            pltpu.VMEM((own_count * n_comm + 1, max(early, 16), max(early, 128)), bf16),
        ]
        + [pltpu.VMEM((own_count + n_comm, size, wide), bf16) for (_, wide, _, size) in pieces]
        + [pltpu.VMEM((peers, size, wide), bf16) for (_, wide, _, size) in pieces]
        + [
            dma((5,)), dma((1,)), dma((count,)), dma((1,)), dma((3,)), dma((1,)), dma((peers,)), dma((peers,)),
            dma((peers, count)), dma((peers, count)), dma((half,)), dma((half,)), dma((half,)), dma((half,)),
            dma((1,)), dma((peers,)), dma((peers,)),
        ],
        compiler_params=pltpu.CompilerParams(
            collective_id=1, has_side_effects=True, vmem_limit_bytes=STEP_VMEM
        ),
        cost_estimate=pl.CostEstimate(flops=1 << 36, bytes_accessed=32 << 20, transcendentals=0),
    )(tile_src, tile_count, request, feats, tiles, z_old, dual, target, w_rows, rho, beta)


def finish_kernel(
    n_wide, rows, column, part, agg_t, agg_last, w_last, scale, target, coef, newz_ref, newdual_ref, moved_ref,
    grads, newz, sems,
):
    own_count, nodes, hidden = part.shape
    _, shard, _ = grads.shape
    half = n_wide // 2
    mine = lax.axis_index("wide") // 2
    j = lax.bitwise_xor(mine, half - 1) if half & (half - 1) == 0 else lax.rem(mine + half - 1, half)
    inverse = coef[...]
    copies = []
    for k in range(own_count):
        for step in range(nodes // rows):
            block = slice(step * rows, (step + 1) * rows)
            agg = agg_last[k, block]
            for n in range(hidden // column):
                cols = slice(n * column, (n + 1) * column)
                gap = mxu(agg, w_last[:, cols]) + part[k, block, cols]
                moved = gap * scale[k, block, cols]
                moved_ref[k, block, cols] = moved.astype(jnp.bfloat16)
                newz[k, block, cols] = (
                    gap + target[k, block, cols].astype(jnp.float32) - moved * inverse[:, cols]
                ).astype(jnp.bfloat16)
            for src, dst in ((newz, newz_ref), (moved_ref, newdual_ref)):
                copy = pltpu.make_async_copy(src.at[k, block], dst.at[k, block], sems.at[len(copies)])
                copy.start()
                copies.append(copy)
    gradient(agg_t, moved_ref, grads, j, column)
    for copy in copies:
        copy.wait()


def gradient(agg_t, moved_ref, grads, j, column):
    own_count, nodes, hidden = moved_ref.shape
    _, shard, _ = grads.shape
    block = pl.ds(pl.multiple_of(j * (2 * shard), 2 * shard), 2 * shard)
    for n in range(hidden // column):
        cols = slice(n * column, (n + 1) * column)
        moved = moved_ref[:, :, cols].reshape(own_count * nodes, column)
        value = mxu(agg_t[block, :], moved).astype(jnp.bfloat16)
        grads[0, :, cols] = value[:shard]
        grads[1, :, cols] = value[shard:]


def finish(part, agg_t, agg_last, w_last, scale, target, coef, n_wide):
    own_count, nodes, hidden = part.shape
    width = agg_t.shape[0]
    rows = largest_block(nodes, 256, 128)
    column = largest_block(hidden, 256, 128)
    vmem = pl.BlockSpec(memory_space=pltpu.VMEM)
    anywhere = pl.BlockSpec(memory_space=pl.ANY)
    bf16 = jnp.bfloat16
    return pl.pallas_call(
        functools.partial(finish_kernel, n_wide, rows, column),
        out_shape=[
            jax.ShapeDtypeStruct(part.shape, bf16),
            jax.ShapeDtypeStruct(part.shape, bf16),
            pltpu.VMEM(part.shape, bf16),
            pltpu.VMEM((2, width // n_wide, hidden), bf16),
        ],
        in_specs=[vmem] * 7,
        out_specs=[pl.BlockSpec(memory_space=pltpu.HBM)] * 2 + [vmem] * 2,
        scratch_shapes=[
            pltpu.VMEM(part.shape, bf16),
            pltpu.SemaphoreType.DMA((2 * own_count * (nodes // rows),)),
        ],
        compiler_params=pltpu.CompilerParams(vmem_limit_bytes=FINISH_VMEM),
        cost_estimate=pl.CostEstimate(flops=1 << 32, bytes_accessed=8 << 20, transcendentals=0),
    )(part, agg_t, agg_last, w_last, scale, target, coef)


def cut(rows):
    direct = 16 if rows % 16 == 0 and rows >= 64 else 0
    rest = rows - direct
    first = rest
    waves = [(0, first)] + ([(first, rest - first)] if first < rest else [])
    return waves, direct


def reduce_kernel(n_comm, n_wide, factor, column, agg_ref, dual_ref, first_ref, out_ref, *refs):
    half = n_wide // 2
    shard, hidden = out_ref.shape
    waves, direct = cut(shard)
    count = len(waves)
    grads, got_pair, pair_send, pair_recv = refs[:4]
    per = [refs[4 + 11 * i : 15 + 11 * i] for i in range(count)]
    columns = hidden // n_comm
    c = lax.axis_index("comm")
    w = lax.axis_index("wide")
    mine = w // 2
    side = lax.rem(w, 2)
    partner = w + 1 - 2 * side
    paired = n_comm & (n_comm - 1) == 0

    def signal(to_c, to_w):
        pl.semaphore_signal(
            pltpu.get_barrier_semaphore(), inc=1, device_id=(to_c, to_w), device_id_type=MESH
        )

    signal(c, partner)
    for off in range(1, half):
        signal(c, lax.rem(mine + off, half) * 2 + side)
    for off in range(1, n_comm):
        signal(lax.rem(c + off, n_comm), w)

    def remote(src, dst, send, recv, to_c, to_w):
        return pltpu.make_async_remote_copy(
            src_ref=src, dst_ref=dst, send_sem=send, recv_sem=recv, device_id=(to_c, to_w),
            device_id_type=MESH,
        )

    def arrived(dst, recv):
        remote(dst, dst, recv, recv, c, partner).wait_recv()

    started = []

    def start(*args):
        copy = remote(*args)
        copy.start()
        started.append(copy)

    def towards(off):
        return lax.bitwise_xor(c, off) if paired else lax.rem(c + off, n_comm)

    def across(off):
        return lax.bitwise_xor(mine, off) if half & (half - 1) == 0 else lax.rem(mine + off, half)

    order = [across(off) for off in range(half - 1, 0, -1)] + [mine]
    far = [n_comm - 1] + list(range(1, n_comm - 1))

    def partial(at):
        return first_ref if at == 0 else grads.at[at - 1]

    def scatter(i, at):
        sums, got_comm, _, _, _, comm_send, comm_recv = per[i][:7]
        for off in far:
            start(
                sums.at[towards(off), at], got_comm.at[c, at], comm_send.at[off - 1, at],
                comm_recv.at[c, at], towards(off), w,
            )

    def combine(at):
        arrived(got_pair.at[at], pair_recv.at[at])
        value = partial(at)[side].astype(jnp.float32) + got_pair[at].astype(jnp.float32)
        value = value.astype(jnp.bfloat16)
        for i, (row, size) in enumerate(waves):
            for q in range(n_comm):
                per[i][0][q, at] = value[row : row + size, q * columns : (q + 1) * columns]
            if i == 0:
                scatter(0, at)
        if direct:
            own, got, _, send, recv = refs[4 + 11 * count :][:5]
            own[at] = value[shard - direct :]
            if at < half - 1:
                start(own.at[at], got.at[mine], send.at[at], recv.at[mine], c, order[at] * 2 + side)

    pl.semaphore_wait(pltpu.get_barrier_semaphore(), 1 + (half - 1) + (n_comm - 1))
    for at, j in enumerate(order):
        if at > 0:
            gradient(agg_ref, dual_ref, grads.at[at - 1], j, column)
        start(
            partial(at).at[1 - side], got_pair.at[at], pair_send.at[at], pair_recv.at[at], c, partner
        )
        if at > 0:
            combine(at - 1)
    combine(half - 1)
    for i in range(1, count):
        for at in range(half):
            scatter(i, at)
    if direct:
        own, got, whole, _, recv, whole_send, whole_recv = refs[4 + 11 * count :]
        total = own[half - 1].astype(jnp.float32)
        for j in order[:-1]:
            arrived(got.at[j], recv.at[j])
            total = total + got[j].astype(jnp.float32)
        whole[c] = total.astype(jnp.bfloat16)
        for off in far:
            start(whole.at[c], whole.at[c], whole_send.at[off - 1], whole_recv.at[c], towards(off), w)
    for i in range(count):
        sums, got_comm, parts, got_wide, final, _, comm_recv, wide_send, wide_recv, final_send, final_recv = per[i]
        for at, j in enumerate(order):
            value = sums[c, at].astype(jnp.float32)
            for off in far:
                q = towards(off)
                arrived(got_comm.at[q, at], comm_recv.at[q, at])
                value = value + got_comm[q, at].astype(jnp.float32)
            if at < half - 1:
                parts[at] = value.astype(jnp.bfloat16)
                start(
                    parts.at[at], got_wide.at[mine], wide_send.at[at], wide_recv.at[mine],
                    c, j * 2 + side,
                )
            else:
                total = value
        for j in order[:-1]:
            arrived(got_wide.at[j], wide_recv.at[j])
            total = total + got_wide[j].astype(jnp.float32)
        final[c] = total.astype(jnp.bfloat16)
        for off in far:
            start(final.at[c], final.at[c], final_send.at[off - 1], final_recv.at[c], towards(off), w)
    if direct:
        for off in far:
            arrived(whole.at[towards(off)], whole_recv.at[towards(off)])
        total = whole[0].astype(jnp.float32)
        for q in range(1, n_comm):
            total = total + whole[q].astype(jnp.float32)
        out_ref[shard - direct :] = total * factor
    for i, (row, size) in enumerate(waves):
        final, final_recv = per[i][4], per[i][10]
        for off in far:
            arrived(final.at[towards(off)], final_recv.at[towards(off)])
        for q in range(n_comm):
            out_ref[row : row + size, q * columns : (q + 1) * columns] = final[q].astype(jnp.float32) * factor
    for copy in started:
        copy.wait_send()


def reduce_grad(agg_t, new_dual, first, n_comm, n_wide, factor):
    width = agg_t.shape[0]
    hidden = new_dual.shape[2]
    rows = width // n_wide
    half = n_wide // 2
    block = (rows, hidden)
    column = largest_block(hidden, 256, 128)
    bf16 = jnp.bfloat16
    dma = pltpu.SemaphoreType.DMA
    waves, direct = cut(rows)
    scratch = [
        pltpu.VMEM((half - 1, 2) + block, bf16), pltpu.VMEM((half,) + block, bf16), dma((half,)), dma((half,)),
    ]
    for _, size in waves:
        piece = (size, hidden // n_comm)
        scratch += [
            pltpu.VMEM((n_comm, half) + piece, bf16), pltpu.VMEM((n_comm, half) + piece, bf16),
            pltpu.VMEM((half,) + piece, bf16), pltpu.VMEM((half,) + piece, bf16),
            pltpu.VMEM((n_comm,) + piece, bf16), dma((n_comm, half)), dma((n_comm, half)), dma((half,)),
            dma((half,)), dma((n_comm,)), dma((n_comm,)),
        ]
    if direct:
        scratch += [
            pltpu.VMEM((half, direct, hidden), bf16), pltpu.VMEM((half, direct, hidden), bf16),
            pltpu.VMEM((n_comm, direct, hidden), bf16), dma((half,)), dma((half,)), dma((n_comm,)), dma((n_comm,)),
        ]
    return pl.pallas_call(
        functools.partial(reduce_kernel, n_comm, n_wide, factor, column),
        out_shape=pltpu.VMEM(block, jnp.float32),
        in_specs=[pl.BlockSpec(memory_space=pltpu.VMEM)] * 3,
        out_specs=pl.BlockSpec(memory_space=pltpu.VMEM),
        scratch_shapes=scratch,
        compiler_params=pltpu.CompilerParams(
            collective_id=0, has_side_effects=True, vmem_limit_bytes=REDUCE_VMEM
        ),
        cost_estimate=pl.CostEstimate(flops=1 << 34, bytes_accessed=8 << 20, transcendentals=0),
    )(agg_t, new_dual, first)


def local(feats, tiles, tile_src, tile_count, request, z_old, dual, target, w_rows, rho, beta):
    own_count, nodes, _ = feats.shape
    hidden = w_rows.shape[1]
    n_comm = lax.axis_size("comm")
    n_wide = lax.axis_size("wide")
    part, agg_t, agg_last, w_last, scale, target, coef = step(
        tile_src, tile_count, request, feats, tiles, z_old, dual, target, w_rows,
        rho.reshape(1, hidden), beta.reshape(1, hidden), n_comm, n_wide,
    )
    new_z, new_dual, moved, first = finish(part, agg_t, agg_last, w_last, scale, target, coef, n_wide)
    factor = 1.0 / math.sqrt(own_count * nodes * n_comm * n_wide)
    return new_z, new_dual, reduce_grad(agg_t, moved, first, n_comm, n_wide, factor)


def solution(mesh):
    in_specs = (
        P(("comm", "wide"), None, None),
        P(("comm", "wide"), None, None, None),
        P(("comm", "wide"), None),
        P(("comm", "wide")),
        P(("comm", "wide"), None),
        P(("comm", "wide"), None, None),
        P(("comm", "wide"), None, None),
        P(("comm", "wide"), None, None),
        P("wide", None),
        P(),
        P(),
    )
    out_specs = (P(("comm", "wide"), None, None), P(("comm", "wide"), None, None), P("wide", None))
    return jax.shard_map(local, mesh=mesh, in_specs=in_specs, out_specs=out_specs, check_vma=False)
```

```python
import functools
import math

import jax
import jax.numpy as jnp
from jax import lax
from jax.experimental import pallas as pl
from jax.experimental.pallas import tpu as pltpu
from jax.sharding import PartitionSpec as P


STEP_VMEM = 40 * 1024 * 1024
FINISH_VMEM = 8 * 1024 * 1024
REDUCE_VMEM = 10 * 1024 * 1024

MESH = pl.DeviceIdType.MESH


def largest_block(size, limit, unit):
    for block in range(limit, 0, -unit):
        if size % block == 0:
            return block
    return size


def mxu(a, b):
    return jnp.dot(a, b, preferred_element_type=jnp.float32)


def pieces_of(nodes, width):
    cw = largest_block(width, 256, 128)
    last = largest_block(nodes, 256, 128)
    early = 128 if cw == 256 and nodes > 128 and width > 2 * cw else 0
    pieces = [(0, early, early, nodes - early), (early, cw - early, 0, nodes)] if early else [(0, cw, 0, nodes)]
    pieces += [(j * cw, cw, 0, nodes) for j in range(1, width // cw - 1)]
    if last < nodes:
        pieces.append((width - cw, cw, 0, nodes - last))
    pieces.append((width - cw, cw, nodes - last if last < nodes else 0, last))
    return cw, early, pieces


def step_kernel(n_comm, n_wide, plan, *refs):
    (cw, early, pieces, rows, column, gather_w) = plan
    count = len(pieces)
    (src_hbm, count_hbm, request_hbm, feats_ref, tiles_ref, z_ref, dual_ref, target_ref, w_ref, rho_ref,
     beta_ref, part, agg_t, agg_last, w_last, scale, target, coef, src_ref, count_ref, request_ref, rates,
     own, tiles, dual, z_old, weight, held, ask, asked, eager) = refs[:31]
    pools = refs[31 : 31 + count]
    stages = refs[31 + count : 31 + 2 * count]
    (small_sem, own_sem, pool_sem, tile_sem, data_sem, w_sem, ask_send, ask_recv, feat_send, feat_recv,
     w_send, w_recv, fwd_send, fwd_recv, eager_sem, eager_send, eager_recv) = refs[31 + 2 * count :]
    own_count, nodes, width = feats_ref.shape
    slots = tiles_ref.shape[1]
    hidden = w_ref.shape[-1]
    peers = n_comm - 1
    paired = n_comm & (n_comm - 1) == 0
    half = n_wide // 2
    dead = own_count + peers
    c = lax.axis_index("comm")
    w = lax.axis_index("wide")
    chip = w // 2
    side = lax.rem(w, 2)
    partner = w + 1 - 2 * side

    def towards(off):
        return lax.bitwise_xor(c, off) if paired else lax.rem(c + off, n_comm)

    def arriving(off):
        return lax.bitwise_xor(c, off) if paired else lax.rem(c - off + n_comm, n_comm)

    def along(off):
        return lax.rem(chip + off, half) * 2 + side

    def signal(to_c, to_w):
        pl.semaphore_signal(
            pltpu.get_barrier_semaphore(), inc=1, device_id=(to_c, to_w), device_id_type=MESH
        )

    def remote(src, dst, send, recv, to_c, to_w):
        return pltpu.make_async_remote_copy(
            src_ref=src, dst_ref=dst, send_sem=send, recv_sem=recv, device_id=(to_c, to_w),
            device_id_type=MESH,
        )

    def arrived(dst, recv):
        remote(dst, dst, recv, recv, c, partner).wait_recv()

    request_copy = pltpu.make_async_copy(request_hbm, request_ref, small_sem.at[0])
    request_copy.start()
    for off in range(1, n_comm):
        signal(lax.rem(c + off, n_comm), w)
    greeted = peers
    if gather_w:
        for off in range(1, half):
            signal(c, along(off))
        signal(c, partner)
        greeted += half
    eager_copy = None
    if early:
        eager_copy = pltpu.make_async_copy(
            feats_ref.at[:, pl.ds(0, early), pl.ds(0, early)], eager.at[pl.ds(0, own_count)], eager_sem.at[0]
        )
        eager_copy.start()
    own_copy = pltpu.make_async_copy(feats_ref, own, own_sem.at[0])
    own_copy.start()
    w_copy = pltpu.make_async_copy(w_ref, weight.at[w] if gather_w else weight, w_sem.at[0])
    w_copy.start()
    small_copies = [
        pltpu.make_async_copy(src_hbm, src_ref, small_sem.at[1]),
        pltpu.make_async_copy(count_hbm, count_ref, small_sem.at[2]),
        pltpu.make_async_copy(rho_ref, rates.at[0], small_sem.at[3]),
        pltpu.make_async_copy(beta_ref, rates.at[1], small_sem.at[4]),
    ]
    pool_copies = [
        pltpu.make_async_copy(
            feats_ref.at[:, pl.ds(row, size), pl.ds(col, wide)], pools[p].at[pl.ds(0, own_count)], pool_sem.at[p]
        )
        for p, (col, wide, row, size) in enumerate(pieces)
    ]
    tile_copy = pltpu.make_async_copy(tiles_ref, tiles, tile_sem.at[0])
    data_copies = [
        pltpu.make_async_copy(dual_ref, dual, data_sem.at[0]),
        pltpu.make_async_copy(target_ref, target, data_sem.at[1]),
        pltpu.make_async_copy(z_ref, z_old, data_sem.at[2]),
    ]
    request_copy.wait()
    for off in range(1, n_comm):
        ask[off - 1] = jnp.full(ask.shape[1:], request_ref[0, arriving(off)], jnp.int32)
    pl.semaphore_wait(pltpu.get_barrier_semaphore(), greeted)

    started = []

    def start(*args):
        copy = remote(*args)
        copy.start()
        started.append(copy)

    near = list(range(1, peers)) + [peers]
    far = [peers] + list(range(1, peers))
    for off in far:
        start(ask.at[off - 1], asked.at[off - 1], ask_send.at[off - 1], ask_recv.at[off - 1], arriving(off), w)
    if early:
        eager_copy.wait()
        for off in far:
            start(
                eager.at[pl.ds(0, own_count)], eager.at[pl.ds(own_count * off, own_count)],
                eager_send.at[off - 1], eager_recv.at[off - 1], towards(off), w,
            )
    for copy in small_copies + pool_copies + [tile_copy] + data_copies:
        copy.start()
    own_copy.wait()
    wants = {}
    for p, (col, wide, row, size) in enumerate(pieces):
        for off in near if p == 0 else far:
            if p == 0:
                arrived(asked.at[off - 1], ask_recv.at[off - 1])
                wants[off] = jnp.clip(jnp.max(asked[off - 1]), 0, own_count - 1)
            stages[p][off - 1] = own[wants[off], row : row + size, col : col + wide]
            start(
                stages[p].at[off - 1], pools[p].at[own_count + off - 1], feat_send.at[off - 1, p],
                feat_recv.at[off - 1, p], towards(off), w,
            )
    w_copy.wait()
    if gather_w:
        for off in range(1, half):
            start(weight.at[w], weight.at[w], w_send.at[off - 1], w_recv.at[chip], c, along(off))
        start(weight.at[w], weight.at[w], fwd_send.at[0], fwd_recv.at[chip], c, partner)
    for p, (_, wide, _, size) in enumerate(pieces):
        pools[p][dead] = jnp.zeros((size, wide), jnp.bfloat16)
    if early:
        eager[own_count * n_comm] = jnp.zeros((early, early), jnp.bfloat16)
    for copy in small_copies:
        copy.wait()

    def pick(k, t):
        source = src_ref[k, t]
        member = jnp.maximum(source - own_count, 0)
        if paired:
            offset = lax.bitwise_xor(c, member)
        else:
            offset = lax.rem(c - member + n_comm, n_comm)
        other = jnp.where(member == c, request_ref[0, c], own_count + offset - 1)
        index = jnp.where(source < own_count, source, other)
        index = jnp.clip(index, 0, dead - 1)
        return jnp.where(t < count_ref[k], index, dead)

    def pick_eager(k, t):
        source = src_ref[k, t]
        member = jnp.clip(source - own_count, 0, peers)
        if paired:
            offset = lax.bitwise_xor(c, member)
        else:
            offset = lax.rem(c - member + n_comm, n_comm)
        index = jnp.where(source < own_count, source, own_count * offset + request_ref[0, member])
        index = jnp.clip(index, 0, own_count * n_comm - 1)
        return jnp.where(t < count_ref[k], index, own_count * n_comm)

    rho = rates[0]
    beta = rates[1]
    inverse = 1.0 / rho
    blend = beta / (rho + beta)
    gain = rho * blend
    coef[0:1] = inverse

    def products(p, k, block):
        (_, _, row, size) = pieces[p]
        total = mxu(tiles[k, 0, block, row : row + size], pools[p][pick(k, 0)])
        for t in range(1, slots):
            total = total + mxu(tiles[k, t, block, row : row + size], pools[p][pick(k, t)])
        if early and p == 0:
            for t in range(slots):
                total = total + mxu(tiles[k, t, block, :early], eager[pick_eager(k, t)])
        return total

    if gather_w:
        for off in range(1, half):
            other = along(off)
            arrived(weight.at[other], w_recv.at[other // 2])
            start(weight.at[other], weight.at[other], fwd_send.at[off], fwd_recv.at[other // 2], c, partner)
        for at in range(half):
            arrived(weight.at[at * 2 + 1 - side], fwd_recv.at[at])
    tile_copy.wait()
    for copy in data_copies:
        copy.wait()

    def w_rows_of(col, wide, cols):
        if gather_w:
            return weight[...].reshape(width, hidden)[col : col + wide, cols]
        return weight[col : col + wide, cols]

    for at in range(hidden // column):
        cols = slice(at * column, (at + 1) * column)
        w_last[:, cols] = w_rows_of(width - cw, cw, cols)

    for p, (col, wide, row, size) in enumerate(pieces):
        pool_copies[p].wait()
        if early and p == 0:
            for off in far:
                arrived(eager.at[pl.ds(own_count * off, own_count)], eager_recv.at[off - 1])
        for off in far:
            arrived(pools[p].at[own_count + off - 1], feat_recv.at[off - 1, p])
        if p == count - 1:
            for k in range(own_count):
                for step in range(nodes // rows):
                    block = slice(step * rows, (step + 1) * rows)
                    total = products(p, k, block)
                    if size < nodes:
                        total = total + held[k, block]
                    agg = total.astype(jnp.bfloat16)
                    agg_last[k, block] = agg
                    at = k * nodes + step * rows
                    agg_t[col : col + cw, at : at + rows] = agg.T
            continue
        steps = nodes // rows

        def body(step, carry, p=p, col=col, wide=wide, steps=steps):
            k = step // steps
            at = lax.rem(step, steps)
            block = pl.ds(pl.multiple_of(at * rows, rows), rows)
            total = products(p, k, block)
            if col == width - cw:
                held[k, block] = total
                return carry
            if p == 0:
                for n in range(hidden // column):
                    cols = slice(n * column, (n + 1) * column)
                    active = z_old[k, block, cols].astype(jnp.float32) > 0
                    scale[k, block, cols] = jnp.where(active, jnp.broadcast_to(gain[:, cols], active.shape), 0.0)
            agg = total.astype(jnp.bfloat16)
            agg_t[col : col + wide, pl.ds(pl.multiple_of(k * nodes + at * rows, 128), rows)] = agg.T
            for n in range(hidden // column):
                cols = slice(n * column, (n + 1) * column)
                value = mxu(agg, w_rows_of(col, wide, cols))
                if p == 0:
                    value = value + (
                        dual[k, block, cols].astype(jnp.float32) * inverse[:, cols]
                        - target[k, block, cols].astype(jnp.float32)
                    )
                else:
                    value = value + part[k, block, cols]
                part[k, block, cols] = value
            return carry

        lax.fori_loop(0, own_count * steps, body, 0)
    for copy in started:
        copy.wait_send()


def step(tile_src, tile_count, request, feats, tiles, z_old, dual, target, w_rows, rho, beta, n_comm, n_wide):
    own_count, nodes, width = feats.shape
    hidden = w_rows.shape[1]
    gather_w = w_rows.shape[0] % 16 == 0
    if not gather_w:
        w_rows = lax.all_gather(w_rows, "wide", axis=0, tiled=True)
    cw, early, pieces = pieces_of(nodes, width)
    column = largest_block(hidden, 256, 128)
    rows = largest_block(nodes, 384, 128)
    plan = (cw, early, pieces, rows, column, gather_w)
    peers = n_comm - 1
    half = n_wide // 2
    count = len(pieces)
    bf16 = jnp.bfloat16
    f32 = jnp.float32
    dma = pltpu.SemaphoreType.DMA
    weight = pltpu.VMEM((n_wide,) + w_rows.shape if gather_w else w_rows.shape, bf16)
    return pl.pallas_call(
        functools.partial(step_kernel, n_comm, n_wide, plan),
        out_shape=[
            pltpu.VMEM(z_old.shape, f32),
            pltpu.VMEM((width, own_count * nodes), bf16),
            pltpu.VMEM((own_count, nodes, cw), bf16),
            pltpu.VMEM((cw, hidden), bf16),
            pltpu.VMEM(z_old.shape, f32),
            pltpu.VMEM(target.shape, bf16),
            pltpu.VMEM((1, hidden), f32),
        ],
        in_specs=[pl.BlockSpec(memory_space=pl.ANY)] * 11,
        out_specs=[pl.BlockSpec(memory_space=pltpu.VMEM)] * 7,
        scratch_shapes=[
            pltpu.SMEM(tile_src.shape, jnp.int32),
            pltpu.SMEM(tile_count.shape, jnp.int32),
            pltpu.SMEM(request.shape, jnp.int32),
            pltpu.VMEM((2, 1, hidden), f32),
            pltpu.VMEM(feats.shape, bf16),
            pltpu.VMEM(tiles.shape, bf16),
            pltpu.VMEM(dual.shape, bf16),
            pltpu.VMEM(z_old.shape, bf16),
            weight,
            pltpu.VMEM((own_count, nodes, cw), f32),
            pltpu.VMEM((peers, 8, 128), jnp.int32),
            pltpu.VMEM((peers, 8, 128), jnp.int32),
            pltpu.VMEM((own_count * n_comm + 1, max(early, 16), max(early, 128)), bf16),
        ]
        + [pltpu.VMEM((own_count + n_comm, size, wide), bf16) for (_, wide, _, size) in pieces]
        + [pltpu.VMEM((peers, size, wide), bf16) for (_, wide, _, size) in pieces]
        + [
            dma((5,)), dma((1,)), dma((count,)), dma((1,)), dma((3,)), dma((1,)), dma((peers,)), dma((peers,)),
            dma((peers, count)), dma((peers, count)), dma((half,)), dma((half,)), dma((half,)), dma((half,)),
            dma((1,)), dma((peers,)), dma((peers,)),
        ],
        compiler_params=pltpu.CompilerParams(
            collective_id=1, has_side_effects=True, vmem_limit_bytes=STEP_VMEM
        ),
        cost_estimate=pl.CostEstimate(flops=1 << 36, bytes_accessed=32 << 20, transcendentals=0),
    )(tile_src, tile_count, request, feats, tiles, z_old, dual, target, w_rows, rho, beta)


def finish_kernel(
    n_wide, rows, column, part, agg_t, agg_last, w_last, scale, target, coef, newz_ref, newdual_ref, moved_ref,
    grads, newz, sems,
):
    own_count, nodes, hidden = part.shape
    inverse = coef[...]
    copies = []
    for k in range(own_count):
        for step in range(nodes // rows):
            block = slice(step * rows, (step + 1) * rows)
            agg = agg_last[k, block]
            for n in range(hidden // column):
                cols = slice(n * column, (n + 1) * column)
                gap = mxu(agg, w_last[:, cols]) + part[k, block, cols]
                moved = gap * scale[k, block, cols]
                moved_ref[k, block, cols] = moved.astype(jnp.bfloat16)
                newz[k, block, cols] = (
                    gap + target[k, block, cols].astype(jnp.float32) - moved * inverse[:, cols]
                ).astype(jnp.bfloat16)
            for src, dst in ((newz, newz_ref), (moved_ref, newdual_ref)):
                copy = pltpu.make_async_copy(src.at[k, block], dst.at[k, block], sems.at[len(copies)])
                copy.start()
                copies.append(copy)
    gradient(agg_t, moved_ref, grads, 0, column)
    for copy in copies:
        copy.wait()


def gradient(agg_t, moved_ref, grads, j, column):
    own_count, nodes, hidden = moved_ref.shape
    _, shard, _ = grads.shape
    block = slice(0, 2 * shard) if isinstance(j, int) else pl.ds(pl.multiple_of(j * (2 * shard), 2 * shard), 2 * shard)
    for n in range(hidden // column):
        cols = slice(n * column, (n + 1) * column)
        moved = moved_ref[:, :, cols].reshape(own_count * nodes, column)
        value = mxu(agg_t[block, :], moved).astype(jnp.bfloat16)
        grads[0, :, cols] = value[:shard]
        grads[1, :, cols] = value[shard:]


def finish(part, agg_t, agg_last, w_last, scale, target, coef, n_wide):
    own_count, nodes, hidden = part.shape
    width = agg_t.shape[0]
    rows = largest_block(nodes, 256, 128)
    column = largest_block(hidden, 256, 128)
    vmem = pl.BlockSpec(memory_space=pltpu.VMEM)
    anywhere = pl.BlockSpec(memory_space=pl.ANY)
    bf16 = jnp.bfloat16
    return pl.pallas_call(
        functools.partial(finish_kernel, n_wide, rows, column),
        out_shape=[
            jax.ShapeDtypeStruct(part.shape, bf16),
            jax.ShapeDtypeStruct(part.shape, bf16),
            pltpu.VMEM(part.shape, bf16),
            pltpu.VMEM((2, width // n_wide, hidden), bf16),
        ],
        in_specs=[vmem] * 7,
        out_specs=[pl.BlockSpec(memory_space=pltpu.HBM)] * 2 + [vmem] * 2,
        scratch_shapes=[
            pltpu.VMEM(part.shape, bf16),
            pltpu.SemaphoreType.DMA((2 * own_count * (nodes // rows),)),
        ],
        compiler_params=pltpu.CompilerParams(vmem_limit_bytes=FINISH_VMEM),
        cost_estimate=pl.CostEstimate(flops=1 << 32, bytes_accessed=8 << 20, transcendentals=0),
    )(part, agg_t, agg_last, w_last, scale, target, coef)


def direct_rows(rows):
    return 16 if rows % 16 == 0 and rows >= 64 else 0


def reduce_kernel(n_comm, n_wide, factor, column, agg_ref, dual_ref, first_ref, out_ref, *refs):
    half = n_wide // 2
    shard, hidden = out_ref.shape
    direct = direct_rows(shard)
    (grads, got_pair, sums, got_comm, parts, got_wide, final, kept, pair_send, pair_recv, comm_send, comm_recv,
     wide_send, wide_recv, final_send, final_recv) = refs[:16]
    if direct:
        whole_own, whole_got, whole, direct_send, direct_recv, whole_send, whole_recv = refs[16:]
    size = shard - direct
    columns = hidden // n_comm
    c = lax.axis_index("comm")
    w = lax.axis_index("wide")
    mine = w // 2
    side = lax.rem(w, 2)
    partner = w + 1 - 2 * side
    paired = n_comm & (n_comm - 1) == 0
    even = half & (half - 1) == 0
    lead = mine == 0
    follow = mine != 0

    def signal(to_c, to_w):
        pl.semaphore_signal(
            pltpu.get_barrier_semaphore(), inc=1, device_id=(to_c, to_w), device_id_type=MESH
        )

    signal(c, partner)
    for off in range(1, half):
        signal(c, lax.rem(mine + off, half) * 2 + side)
    for off in range(1, n_comm):
        signal(lax.rem(c + off, n_comm), w)

    def remote(src, dst, send, recv, to_c, to_w):
        return pltpu.make_async_remote_copy(
            src_ref=src, dst_ref=dst, send_sem=send, recv_sem=recv, device_id=(to_c, to_w),
            device_id_type=MESH,
        )

    def arrived(dst, recv):
        remote(dst, dst, recv, recv, c, partner).wait_recv()

    started = []

    def start(*args, when=None):
        copy = remote(*args)
        started.append((copy, when))
        if when is None:
            copy.start()
        else:
            pl.when(when)(copy.start)

    def towards(off):
        return lax.bitwise_xor(c, off) if paired else lax.rem(c + off, n_comm)

    def across(off):
        return lax.bitwise_xor(mine, off) if even else lax.rem(mine + off, half)

    place = half - 1 - mine if even else jnp.where(lead, half - 1, mine - 1)
    listed = [across(off) for off in range(half - 1, 0, -1)] + [mine]
    order = [0] + [jnp.where(at - 1 < place, listed[at - 1], listed[at]) for at in range(1, half)]
    far = [n_comm - 1] + list(range(1, n_comm - 1))

    def elsewhere(at):
        return follow if at == 0 else lead if at == half - 1 else None

    def partial(at):
        return first_ref if at == 0 else grads.at[at - 1]

    def combine(at):
        arrived(got_pair.at[at], pair_recv.at[at])
        value = partial(at)[side].astype(jnp.float32) + got_pair[at].astype(jnp.float32)
        value = value.astype(jnp.bfloat16)
        for q in range(n_comm):
            sums[q, at] = value[:size, q * columns : (q + 1) * columns]
        for off in far:
            start(
                sums.at[towards(off), at], got_comm.at[c, at], comm_send.at[off - 1, at],
                comm_recv.at[c, at], towards(off), w,
            )
        if direct:
            whole_own[at] = value[size:]
            start(
                whole_own.at[at], whole_got.at[mine], direct_send.at[at], direct_recv.at[mine],
                c, order[at] * 2 + side, when=elsewhere(at),
            )

    pl.semaphore_wait(pltpu.get_barrier_semaphore(), 1 + (half - 1) + (n_comm - 1))
    for at, j in enumerate(order):
        if at > 0:
            gradient(agg_ref, dual_ref, grads.at[at - 1], j, column)
        start(
            partial(at).at[1 - side], got_pair.at[at], pair_send.at[at], pair_recv.at[at], c, partner
        )
        if at > 0:
            combine(at - 1)
    combine(half - 1)

    finals = [
        remote(final.at[c], final.at[c], final_send.at[off - 1], final_recv.at[c], towards(off), w) for off in far
    ]

    def conclude():
        total = kept[...]
        for off in range(1, half):
            j = across(off)
            arrived(got_wide.at[j], wide_recv.at[j])
            total = total + got_wide[j].astype(jnp.float32)
        final[c] = total.astype(jnp.bfloat16)
        for copy in finals:
            copy.start()

    for at, j in enumerate(order):
        value = sums[c, at].astype(jnp.float32)
        for off in far:
            q = towards(off)
            arrived(got_comm.at[q, at], comm_recv.at[q, at])
            value = value + got_comm[q, at].astype(jnp.float32)
        if at == 0 or at == half - 1:

            @pl.when(lead if at == 0 else follow)
            def _(value=value):
                kept[...] = value

        parts[at] = value.astype(jnp.bfloat16)
        start(
            parts.at[at], got_wide.at[mine], wide_send.at[at], wide_recv.at[mine], c, j * 2 + side,
            when=elsewhere(at),
        )
        if at == min(2, half - 1):
            pl.when(lead)(conclude)
        if direct and at == 0:
            total = whole_own[jnp.where(lead, 0, half - 1)].astype(jnp.float32)
            for off in range(1, half):
                other = across(off)
                arrived(whole_got.at[other], direct_recv.at[other])
                total = total + whole_got[other].astype(jnp.float32)
            whole[c] = total.astype(jnp.bfloat16)
            for off in far:
                start(whole.at[c], whole.at[c], whole_send.at[off - 1], whole_recv.at[c], towards(off), w)
    pl.when(follow)(conclude)
    if direct:
        for off in far:
            arrived(whole.at[towards(off)], whole_recv.at[towards(off)])
        total = whole[0].astype(jnp.float32)
        for q in range(1, n_comm):
            total = total + whole[q].astype(jnp.float32)
        out_ref[size:] = total * factor
    for off in far:
        arrived(final.at[towards(off)], final_recv.at[towards(off)])
    for q in range(n_comm):
        out_ref[:size, q * columns : (q + 1) * columns] = final[q].astype(jnp.float32) * factor
    for copy, when in started + [(copy, None) for copy in finals]:
        if when is None:
            copy.wait_send()
        else:
            pl.when(when)(copy.wait_send)


def reduce_grad(agg_t, new_dual, first, n_comm, n_wide, factor):
    width = agg_t.shape[0]
    hidden = new_dual.shape[2]
    rows = width // n_wide
    half = n_wide // 2
    block = (rows, hidden)
    column = largest_block(hidden, 256, 128)
    bf16 = jnp.bfloat16
    dma = pltpu.SemaphoreType.DMA
    direct = direct_rows(rows)
    piece = (rows - direct, hidden // n_comm)
    scratch = [
        pltpu.VMEM((half - 1, 2) + block, bf16), pltpu.VMEM((half,) + block, bf16),
        pltpu.VMEM((n_comm, half) + piece, bf16), pltpu.VMEM((n_comm, half) + piece, bf16),
        pltpu.VMEM((half,) + piece, bf16), pltpu.VMEM((half,) + piece, bf16), pltpu.VMEM((n_comm,) + piece, bf16),
        pltpu.VMEM(piece, jnp.float32), dma((half,)), dma((half,)), dma((n_comm, half)), dma((n_comm, half)),
        dma((half,)), dma((half,)), dma((n_comm,)), dma((n_comm,)),
    ]
    if direct:
        scratch += [
            pltpu.VMEM((half, direct, hidden), bf16), pltpu.VMEM((half, direct, hidden), bf16),
            pltpu.VMEM((n_comm, direct, hidden), bf16), dma((half,)), dma((half,)), dma((n_comm,)), dma((n_comm,)),
        ]
    return pl.pallas_call(
        functools.partial(reduce_kernel, n_comm, n_wide, factor, column),
        out_shape=pltpu.VMEM(block, jnp.float32),
        in_specs=[pl.BlockSpec(memory_space=pltpu.VMEM)] * 3,
        out_specs=pl.BlockSpec(memory_space=pltpu.VMEM),
        scratch_shapes=scratch,
        compiler_params=pltpu.CompilerParams(
            collective_id=0, has_side_effects=True, vmem_limit_bytes=REDUCE_VMEM
        ),
        cost_estimate=pl.CostEstimate(flops=1 << 34, bytes_accessed=8 << 20, transcendentals=0),
    )(agg_t, new_dual, first)


def local(feats, tiles, tile_src, tile_count, request, z_old, dual, target, w_rows, rho, beta):
    own_count, nodes, _ = feats.shape
    hidden = w_rows.shape[1]
    n_comm = lax.axis_size("comm")
    n_wide = lax.axis_size("wide")
    part, agg_t, agg_last, w_last, scale, target, coef = step(
        tile_src, tile_count, request, feats, tiles, z_old, dual, target, w_rows,
        rho.reshape(1, hidden), beta.reshape(1, hidden), n_comm, n_wide,
    )
    new_z, new_dual, moved, first = finish(part, agg_t, agg_last, w_last, scale, target, coef, n_wide)
    factor = 1.0 / math.sqrt(own_count * nodes * n_comm * n_wide)
    return new_z, new_dual, reduce_grad(agg_t, moved, first, n_comm, n_wide, factor)


def solution(mesh):
    in_specs = (
        P(("comm", "wide"), None, None),
        P(("comm", "wide"), None, None, None),
        P(("comm", "wide"), None),
        P(("comm", "wide")),
        P(("comm", "wide"), None),
        P(("comm", "wide"), None, None),
        P(("comm", "wide"), None, None),
        P(("comm", "wide"), None, None),
        P("wide", None),
        P(),
        P(),
    )
    out_specs = (P(("comm", "wide"), None, None), P(("comm", "wide"), None, None), P("wide", None))
    return jax.shard_map(local, mesh=mesh, in_specs=in_specs, out_specs=out_specs, check_vma=False)
```

```python
import functools
import math

import jax
import jax.numpy as jnp
from jax import lax
from jax.experimental import pallas as pl
from jax.experimental.pallas import tpu as pltpu
from jax.sharding import PartitionSpec as P


STEP_VMEM = 40 * 1024 * 1024
FINISH_VMEM = 8 * 1024 * 1024
REDUCE_VMEM = 10 * 1024 * 1024

MESH = pl.DeviceIdType.MESH


def largest_block(size, limit, unit):
    for block in range(limit, 0, -unit):
        if size % block == 0:
            return block
    return size


def mxu(a, b):
    return jnp.dot(a, b, preferred_element_type=jnp.float32)


def pieces_of(nodes, width):
    cw = largest_block(width, 256, 128)
    last = largest_block(nodes, 256, 128)
    early = 128 if cw == 256 and nodes > 128 and width > 2 * cw else 0
    pieces = [(0, early, early, nodes - early), (early, cw - early, 0, nodes)] if early else [(0, cw, 0, nodes)]
    pieces += [(j * cw, cw, 0, nodes) for j in range(1, width // cw - 1)]
    if last < nodes:
        pieces.append((width - cw, cw, 0, nodes - last))
    pieces.append((width - cw, cw, nodes - last if last < nodes else 0, last))
    return cw, early, pieces


def step_kernel(n_comm, n_wide, plan, *refs):
    (cw, early, pieces, rows, column, gather_w) = plan
    count = len(pieces)
    (src_hbm, count_hbm, request_hbm, feats_ref, tiles_ref, z_ref, dual_ref, target_ref, w_ref, rho_ref,
     beta_ref, part, agg_t, agg_last, w_last, scale, target, coef, src_ref, count_ref, request_ref, rates,
     own, tiles, dual, z_old, weight, held, ask, asked, eager) = refs[:31]
    pools = refs[31 : 31 + count]
    stages = refs[31 + count : 31 + 2 * count]
    (small_sem, own_sem, pool_sem, tile_sem, data_sem, w_sem, ask_send, ask_recv, feat_send, feat_recv,
     w_send, w_recv, fwd_send, fwd_recv, eager_sem, eager_send, eager_recv) = refs[31 + 2 * count :]
    own_count, nodes, width = feats_ref.shape
    slots = tiles_ref.shape[1]
    hidden = w_ref.shape[-1]
    peers = n_comm - 1
    paired = n_comm & (n_comm - 1) == 0
    half = n_wide // 2
    dead = own_count + peers
    c = lax.axis_index("comm")
    w = lax.axis_index("wide")
    chip = w // 2
    side = lax.rem(w, 2)
    partner = w + 1 - 2 * side

    def towards(off):
        return lax.bitwise_xor(c, off) if paired else lax.rem(c + off, n_comm)

    def arriving(off):
        return lax.bitwise_xor(c, off) if paired else lax.rem(c - off + n_comm, n_comm)

    def along(off):
        return lax.rem(chip + off, half) * 2 + side

    def signal(to_c, to_w):
        pl.semaphore_signal(
            pltpu.get_barrier_semaphore(), inc=1, device_id=(to_c, to_w), device_id_type=MESH
        )

    def remote(src, dst, send, recv, to_c, to_w):
        return pltpu.make_async_remote_copy(
            src_ref=src, dst_ref=dst, send_sem=send, recv_sem=recv, device_id=(to_c, to_w),
            device_id_type=MESH,
        )

    def arrived(dst, recv):
        remote(dst, dst, recv, recv, c, partner).wait_recv()

    request_copy = pltpu.make_async_copy(request_hbm, request_ref, small_sem.at[0])
    request_copy.start()
    for off in range(1, n_comm):
        signal(lax.rem(c + off, n_comm), w)
    greeted = peers
    if gather_w:
        for off in range(1, half):
            signal(c, along(off))
        signal(c, partner)
        greeted += half
    eager_copy = None
    if early:
        eager_copy = pltpu.make_async_copy(
            feats_ref.at[:, pl.ds(0, early), pl.ds(0, early)], eager.at[pl.ds(0, own_count)], eager_sem.at[0]
        )
        eager_copy.start()
    own_copy = pltpu.make_async_copy(feats_ref, own, own_sem.at[0])
    own_copy.start()
    w_copy = pltpu.make_async_copy(w_ref, weight.at[w] if gather_w else weight, w_sem.at[0])
    w_copy.start()
    small_copies = [
        pltpu.make_async_copy(src_hbm, src_ref, small_sem.at[1]),
        pltpu.make_async_copy(count_hbm, count_ref, small_sem.at[2]),
        pltpu.make_async_copy(rho_ref, rates.at[0], small_sem.at[3]),
        pltpu.make_async_copy(beta_ref, rates.at[1], small_sem.at[4]),
    ]
    pool_copies = [
        pltpu.make_async_copy(
            feats_ref.at[:, pl.ds(row, size), pl.ds(col, wide)], pools[p].at[pl.ds(0, own_count)], pool_sem.at[p]
        )
        for p, (col, wide, row, size) in enumerate(pieces)
    ]
    tile_copy = pltpu.make_async_copy(tiles_ref, tiles, tile_sem.at[0])
    data_copies = [
        pltpu.make_async_copy(dual_ref, dual, data_sem.at[0]),
        pltpu.make_async_copy(target_ref, target, data_sem.at[1]),
        pltpu.make_async_copy(z_ref, z_old, data_sem.at[2]),
    ]
    request_copy.wait()
    for off in range(1, n_comm):
        ask[off - 1] = jnp.full(ask.shape[1:], request_ref[0, arriving(off)], jnp.int32)
    pl.semaphore_wait(pltpu.get_barrier_semaphore(), greeted)

    started = []

    def start(*args):
        copy = remote(*args)
        copy.start()
        started.append(copy)

    near = list(range(1, peers)) + [peers]
    far = [peers] + list(range(1, peers))
    for off in far:
        start(ask.at[off - 1], asked.at[off - 1], ask_send.at[off - 1], ask_recv.at[off - 1], arriving(off), w)
    if early:
        eager_copy.wait()
        for off in far:
            start(
                eager.at[pl.ds(0, own_count)], eager.at[pl.ds(own_count * off, own_count)],
                eager_send.at[off - 1], eager_recv.at[off - 1], towards(off), w,
            )
    for copy in small_copies + pool_copies + [tile_copy] + data_copies:
        copy.start()
    own_copy.wait()
    wants = {}
    for p, (col, wide, row, size) in enumerate(pieces):
        for off in near if p == 0 else far:
            if p == 0:
                arrived(asked.at[off - 1], ask_recv.at[off - 1])
                wants[off] = jnp.clip(jnp.max(asked[off - 1]), 0, own_count - 1)
            stages[p][off - 1] = own[wants[off], row : row + size, col : col + wide]
            start(
                stages[p].at[off - 1], pools[p].at[own_count + off - 1], feat_send.at[off - 1, p],
                feat_recv.at[off - 1, p], towards(off), w,
            )
    w_copy.wait()
    if gather_w:
        for off in range(1, half):
            start(weight.at[w], weight.at[w], w_send.at[off - 1], w_recv.at[chip], c, along(off))
        start(weight.at[w], weight.at[w], fwd_send.at[0], fwd_recv.at[chip], c, partner)
    for p, (_, wide, _, size) in enumerate(pieces):
        pools[p][dead] = jnp.zeros((size, wide), jnp.bfloat16)
    if early:
        eager[own_count * n_comm] = jnp.zeros((early, early), jnp.bfloat16)
    for copy in small_copies:
        copy.wait()

    def pick(k, t):
        source = src_ref[k, t]
        member = jnp.maximum(source - own_count, 0)
        if paired:
            offset = lax.bitwise_xor(c, member)
        else:
            offset = lax.rem(c - member + n_comm, n_comm)
        other = jnp.where(member == c, request_ref[0, c], own_count + offset - 1)
        index = jnp.where(source < own_count, source, other)
        index = jnp.clip(index, 0, dead - 1)
        return jnp.where(t < count_ref[k], index, dead)

    def pick_eager(k, t):
        source = src_ref[k, t]
        member = jnp.clip(source - own_count, 0, peers)
        if paired:
            offset = lax.bitwise_xor(c, member)
        else:
            offset = lax.rem(c - member + n_comm, n_comm)
        index = jnp.where(source < own_count, source, own_count * offset + request_ref[0, member])
        index = jnp.clip(index, 0, own_count * n_comm - 1)
        return jnp.where(t < count_ref[k], index, own_count * n_comm)

    rho = rates[0]
    beta = rates[1]
    inverse = 1.0 / rho
    blend = beta / (rho + beta)
    gain = rho * blend
    coef[0:1] = inverse

    def products(p, k, block):
        (_, _, row, size) = pieces[p]
        total = mxu(tiles[k, 0, block, row : row + size], pools[p][pick(k, 0)])
        for t in range(1, slots):
            total = total + mxu(tiles[k, t, block, row : row + size], pools[p][pick(k, t)])
        if early and p == 0:
            for t in range(slots):
                total = total + mxu(tiles[k, t, block, :early], eager[pick_eager(k, t)])
        return total

    if gather_w:
        for off in range(1, half):
            other = along(off)
            arrived(weight.at[other], w_recv.at[other // 2])
            start(weight.at[other], weight.at[other], fwd_send.at[off], fwd_recv.at[other // 2], c, partner)
        for at in range(half):
            arrived(weight.at[at * 2 + 1 - side], fwd_recv.at[at])
    tile_copy.wait()
    for copy in data_copies:
        copy.wait()

    def w_rows_of(col, wide, cols):
        if gather_w:
            return weight[...].reshape(width, hidden)[col : col + wide, cols]
        return weight[col : col + wide, cols]

    for at in range(hidden // column):
        cols = slice(at * column, (at + 1) * column)
        w_last[:, cols] = w_rows_of(width - cw, cw, cols)

    for p, (col, wide, row, size) in enumerate(pieces):
        pool_copies[p].wait()
        if early and p == 0:
            for off in far:
                arrived(eager.at[pl.ds(own_count * off, own_count)], eager_recv.at[off - 1])
        for off in far:
            arrived(pools[p].at[own_count + off - 1], feat_recv.at[off - 1, p])
        if p == count - 1:
            for k in range(own_count):
                for step in range(nodes // rows):
                    block = slice(step * rows, (step + 1) * rows)
                    total = products(p, k, block)
                    if size < nodes:
                        total = total + held[k, block]
                    agg = total.astype(jnp.bfloat16)
                    agg_last[k, block] = agg
                    at = k * nodes + step * rows
                    agg_t[col : col + cw, at : at + rows] = agg.T
            continue
        steps = nodes // rows

        def body(step, carry, p=p, col=col, wide=wide, steps=steps):
            k = step // steps
            at = lax.rem(step, steps)
            block = pl.ds(pl.multiple_of(at * rows, rows), rows)
            total = products(p, k, block)
            if col == width - cw:
                held[k, block] = total
                return carry
            if p == 0:
                for n in range(hidden // column):
                    cols = slice(n * column, (n + 1) * column)
                    active = z_old[k, block, cols].astype(jnp.float32) > 0
                    scale[k, block, cols] = jnp.where(active, jnp.broadcast_to(gain[:, cols], active.shape), 0.0)
            agg = total.astype(jnp.bfloat16)
            agg_t[col : col + wide, pl.ds(pl.multiple_of(k * nodes + at * rows, 128), rows)] = agg.T
            for n in range(hidden // column):
                cols = slice(n * column, (n + 1) * column)
                value = mxu(agg, w_rows_of(col, wide, cols))
                if p == 0:
                    value = value + (
                        dual[k, block, cols].astype(jnp.float32) * inverse[:, cols]
                        - target[k, block, cols].astype(jnp.float32)
                    )
                else:
                    value = value + part[k, block, cols]
                part[k, block, cols] = value
            return carry

        lax.fori_loop(0, own_count * steps, body, 0)
    for copy in started:
        copy.wait_send()


def step(tile_src, tile_count, request, feats, tiles, z_old, dual, target, w_rows, rho, beta, n_comm, n_wide):
    own_count, nodes, width = feats.shape
    hidden = w_rows.shape[1]
    gather_w = w_rows.shape[0] % 16 == 0
    if not gather_w:
        w_rows = lax.all_gather(w_rows, "wide", axis=0, tiled=True)
    cw, early, pieces = pieces_of(nodes, width)
    column = largest_block(hidden, 256, 128)
    rows = largest_block(nodes, 384, 128)
    plan = (cw, early, pieces, rows, column, gather_w)
    peers = n_comm - 1
    half = n_wide // 2
    count = len(pieces)
    bf16 = jnp.bfloat16
    f32 = jnp.float32
    dma = pltpu.SemaphoreType.DMA
    weight = pltpu.VMEM((n_wide,) + w_rows.shape if gather_w else w_rows.shape, bf16)
    return pl.pallas_call(
        functools.partial(step_kernel, n_comm, n_wide, plan),
        out_shape=[
            pltpu.VMEM(z_old.shape, f32),
            pltpu.VMEM((width, own_count * nodes), bf16),
            pltpu.VMEM((own_count, nodes, cw), bf16),
            pltpu.VMEM((cw, hidden), bf16),
            pltpu.VMEM(z_old.shape, f32),
            pltpu.VMEM(target.shape, bf16),
            pltpu.VMEM((1, hidden), f32),
        ],
        in_specs=[pl.BlockSpec(memory_space=pl.ANY)] * 11,
        out_specs=[pl.BlockSpec(memory_space=pltpu.VMEM)] * 7,
        scratch_shapes=[
            pltpu.SMEM(tile_src.shape, jnp.int32),
            pltpu.SMEM(tile_count.shape, jnp.int32),
            pltpu.SMEM(request.shape, jnp.int32),
            pltpu.VMEM((2, 1, hidden), f32),
            pltpu.VMEM(feats.shape, bf16),
            pltpu.VMEM(tiles.shape, bf16),
            pltpu.VMEM(dual.shape, bf16),
            pltpu.VMEM(z_old.shape, bf16),
            weight,
            pltpu.VMEM((own_count, nodes, cw), f32),
            pltpu.VMEM((peers, 8, 128), jnp.int32),
            pltpu.VMEM((peers, 8, 128), jnp.int32),
            pltpu.VMEM((own_count * n_comm + 1, max(early, 16), max(early, 128)), bf16),
        ]
        + [pltpu.VMEM((own_count + n_comm, size, wide), bf16) for (_, wide, _, size) in pieces]
        + [pltpu.VMEM((peers, size, wide), bf16) for (_, wide, _, size) in pieces]
        + [
            dma((5,)), dma((1,)), dma((count,)), dma((1,)), dma((3,)), dma((1,)), dma((peers,)), dma((peers,)),
            dma((peers, count)), dma((peers, count)), dma((half,)), dma((half,)), dma((half,)), dma((half,)),
            dma((1,)), dma((peers,)), dma((peers,)),
        ],
        compiler_params=pltpu.CompilerParams(
            collective_id=1, has_side_effects=True, vmem_limit_bytes=STEP_VMEM
        ),
        cost_estimate=pl.CostEstimate(flops=1 << 36, bytes_accessed=32 << 20, transcendentals=0),
    )(tile_src, tile_count, request, feats, tiles, z_old, dual, target, w_rows, rho, beta)


def finish_kernel(
    n_wide, rows, column, part, agg_t, agg_last, w_last, scale, target, coef, newz_ref, newdual_ref, moved_ref,
    grads, newz, sems,
):
    own_count, nodes, hidden = part.shape
    inverse = coef[...]
    copies = []
    for k in range(own_count):
        for step in range(nodes // rows):
            block = slice(step * rows, (step + 1) * rows)
            agg = agg_last[k, block]
            for n in range(hidden // column):
                cols = slice(n * column, (n + 1) * column)
                gap = mxu(agg, w_last[:, cols]) + part[k, block, cols]
                moved = gap * scale[k, block, cols]
                moved_ref[k, block, cols] = moved.astype(jnp.bfloat16)
                newz[k, block, cols] = (
                    gap + target[k, block, cols].astype(jnp.float32) - moved * inverse[:, cols]
                ).astype(jnp.bfloat16)
            for src, dst in ((newz, newz_ref), (moved_ref, newdual_ref)):
                copy = pltpu.make_async_copy(src.at[k, block], dst.at[k, block], sems.at[len(copies)])
                copy.start()
                copies.append(copy)
    j = jnp.where(lax.axis_index("wide") // 2 == 0, 1, 0)
    gradient(agg_t, moved_ref, grads, j, column)
    for copy in copies:
        copy.wait()


def gradient(agg_t, moved_ref, grads, j, column):
    own_count, nodes, hidden = moved_ref.shape
    _, shard, _ = grads.shape
    block = slice(0, 2 * shard) if isinstance(j, int) else pl.ds(pl.multiple_of(j * (2 * shard), 2 * shard), 2 * shard)
    for n in range(hidden // column):
        cols = slice(n * column, (n + 1) * column)
        moved = moved_ref[:, :, cols].reshape(own_count * nodes, column)
        value = mxu(agg_t[block, :], moved).astype(jnp.bfloat16)
        grads[0, :, cols] = value[:shard]
        grads[1, :, cols] = value[shard:]


def finish(part, agg_t, agg_last, w_last, scale, target, coef, n_wide):
    own_count, nodes, hidden = part.shape
    width = agg_t.shape[0]
    rows = largest_block(nodes, 256, 128)
    column = largest_block(hidden, 256, 128)
    vmem = pl.BlockSpec(memory_space=pltpu.VMEM)
    anywhere = pl.BlockSpec(memory_space=pl.ANY)
    bf16 = jnp.bfloat16
    return pl.pallas_call(
        functools.partial(finish_kernel, n_wide, rows, column),
        out_shape=[
            jax.ShapeDtypeStruct(part.shape, bf16),
            jax.ShapeDtypeStruct(part.shape, bf16),
            pltpu.VMEM(part.shape, bf16),
            pltpu.VMEM((2, width // n_wide, hidden), bf16),
        ],
        in_specs=[vmem] * 7,
        out_specs=[pl.BlockSpec(memory_space=pltpu.HBM)] * 2 + [vmem] * 2,
        scratch_shapes=[
            pltpu.VMEM(part.shape, bf16),
            pltpu.SemaphoreType.DMA((2 * own_count * (nodes // rows),)),
        ],
        compiler_params=pltpu.CompilerParams(vmem_limit_bytes=FINISH_VMEM),
        cost_estimate=pl.CostEstimate(flops=1 << 32, bytes_accessed=8 << 20, transcendentals=0),
    )(part, agg_t, agg_last, w_last, scale, target, coef)


def direct_rows(rows):
    return 16 if rows % 16 == 0 and rows >= 64 else 0


def reduce_kernel(n_comm, n_wide, factor, column, agg_ref, dual_ref, first_ref, out_ref, *refs):
    half = n_wide // 2
    shard, hidden = out_ref.shape
    direct = direct_rows(shard)
    (grads, got_pair, sums, got_comm, parts, got_wide, final, early_own, early_got, pair_send, pair_recv, comm_send, comm_recv,
     wide_send, wide_recv, final_send, final_recv, early_send, early_recv) = refs[:19]
    if direct:
        whole_own, whole_got, whole, direct_send, direct_recv, whole_send, whole_recv = refs[19:]
    size = shard - direct
    columns = hidden // n_comm
    c = lax.axis_index("comm")
    w = lax.axis_index("wide")
    mine = w // 2
    side = lax.rem(w, 2)
    partner = w + 1 - 2 * side
    paired = n_comm & (n_comm - 1) == 0
    even = half & (half - 1) == 0
    lead = mine == 0
    follow = mine != 0

    def signal(to_c, to_w):
        pl.semaphore_signal(
            pltpu.get_barrier_semaphore(), inc=1, device_id=(to_c, to_w), device_id_type=MESH
        )

    signal(c, partner)
    for off in range(1, half):
        signal(c, lax.rem(mine + off, half) * 2 + side)
    for off in range(1, n_comm):
        signal(lax.rem(c + off, n_comm), w)

    def remote(src, dst, send, recv, to_c, to_w):
        return pltpu.make_async_remote_copy(
            src_ref=src, dst_ref=dst, send_sem=send, recv_sem=recv, device_id=(to_c, to_w),
            device_id_type=MESH,
        )

    def arrived(dst, recv):
        remote(dst, dst, recv, recv, c, partner).wait_recv()

    started = []

    def start(*args, when=None):
        copy = remote(*args)
        started.append((copy, when))
        if when is None:
            copy.start()
        else:
            pl.when(when)(copy.start)

    def towards(off):
        return lax.bitwise_xor(c, off) if paired else lax.rem(c + off, n_comm)

    def across(off):
        return lax.bitwise_xor(mine, off) if even else lax.rem(mine + off, half)

    place = half - 1 - mine if even else mine - 1
    listed = [across(off) for off in range(half - 1, 0, -1)] + [mine]
    order = [0] + [jnp.where(at - 1 < place, listed[at - 1], listed[at]) for at in range(1, half)]
    leading = [listed[half - 2]] + listed[: half - 2] + [mine]
    order = [jnp.where(lead, leading[at], order[at]) for at in range(half)]
    far = [n_comm - 1] + list(range(1, n_comm - 1))

    def partial(at):
        return first_ref if at == 0 else grads.at[at - 1]

    def combine(at):
        arrived(got_pair.at[at], pair_recv.at[at])
        value = partial(at)[side].astype(jnp.float32) + got_pair[at].astype(jnp.float32)
        head = value[:size]
        if at == half - 1:

            @pl.when(mine == 1)
            def _():
                arrived(early_got, early_recv.at[0])

            head = head + early_got[...].astype(jnp.float32)
        head = head.astype(jnp.bfloat16)
        for q in range(n_comm):
            sums[q, at] = head[:, q * columns : (q + 1) * columns]
        for off in far:
            start(
                sums.at[towards(off), at], got_comm.at[c, at], comm_send.at[off - 1, at],
                comm_recv.at[c, at], towards(off), w, when=follow if at == 0 else None,
            )
        if at == 0:
            early_own[...] = head
            start(early_own, early_got, early_send.at[0], early_recv.at[0], c, 2 + side, when=lead)
        if direct:
            whole_own[at] = value[size:].astype(jnp.bfloat16)
            if at < half - 1:
                start(
                    whole_own.at[at], whole_got.at[mine], direct_send.at[at], direct_recv.at[mine],
                    c, order[at] * 2 + side,
                )

    @pl.when(mine != 1)
    def _():
        early_got[...] = jnp.zeros_like(early_got)

    @pl.when(mine == 1)
    def _():
        got_wide[0] = jnp.zeros(got_wide.shape[1:], jnp.bfloat16)

    pl.semaphore_wait(pltpu.get_barrier_semaphore(), 1 + (half - 1) + (n_comm - 1))
    for at, j in enumerate(order):
        if at > 0:
            gradient(agg_ref, dual_ref, grads.at[at - 1], j, column)
        start(
            partial(at).at[1 - side], got_pair.at[at], pair_send.at[at], pair_recv.at[at], c, partner
        )
        if at > 0:
            combine(at - 1)

    finals = [
        remote(final.at[c], final.at[c], final_send.at[off - 1], final_recv.at[c], towards(off), w) for off in far
    ]

    def received(at):
        value = sums[c, at].astype(jnp.float32)
        for off in far:
            q = towards(off)
            arrived(got_comm.at[q, at], comm_recv.at[q, at])
            value = value + got_comm[q, at].astype(jnp.float32)
        return value

    wides = [
        remote(parts.at[at], got_wide.at[mine], wide_send.at[at], wide_recv.at[mine], c, order[at] * 2 + side)
        for at in range(half - 1)
    ]

    def forward(at):
        parts[at] = received(at).astype(jnp.bfloat16)
        wides[at].start()

    for at in range(half - 1):
        if at == 0:
            pl.when(follow)(functools.partial(forward, 0))
            combine(half - 1)
        else:
            forward(at)
        if direct and at == 0:
            total = whole_own[half - 1].astype(jnp.float32)
            for off in range(1, half):
                other = across(off)
                arrived(whole_got.at[other], direct_recv.at[other])
                total = total + whole_got[other].astype(jnp.float32)
            whole[c] = total.astype(jnp.bfloat16)
            for off in far:
                start(whole.at[c], whole.at[c], whole_send.at[off - 1], whole_recv.at[c], towards(off), w)
    total = received(half - 1)
    for off in range(1, half):
        other = across(off)

        @pl.when(jnp.logical_not(jnp.logical_and(mine == 1, other == 0)))
        def _(other=other):
            arrived(got_wide.at[other], wide_recv.at[other])

        total = total + got_wide[other].astype(jnp.float32)
    final[c] = total.astype(jnp.bfloat16)
    for copy in finals:
        copy.start()
    if direct:
        for off in far:
            arrived(whole.at[towards(off)], whole_recv.at[towards(off)])
        total = whole[0].astype(jnp.float32)
        for q in range(1, n_comm):
            total = total + whole[q].astype(jnp.float32)
        out_ref[size:] = total * factor
    for off in far:
        arrived(final.at[towards(off)], final_recv.at[towards(off)])
    for q in range(n_comm):
        out_ref[:size, q * columns : (q + 1) * columns] = final[q].astype(jnp.float32) * factor
    waits = started + [(copy, None) for copy in finals]
    waits += [(copy, follow if at == 0 else None) for at, copy in enumerate(wides)]
    for copy, when in waits:
        if when is None:
            copy.wait_send()
        else:
            pl.when(when)(copy.wait_send)


def reduce_grad(agg_t, new_dual, first, n_comm, n_wide, factor):
    width = agg_t.shape[0]
    hidden = new_dual.shape[2]
    rows = width // n_wide
    half = n_wide // 2
    block = (rows, hidden)
    column = largest_block(hidden, 256, 128)
    bf16 = jnp.bfloat16
    dma = pltpu.SemaphoreType.DMA
    direct = direct_rows(rows)
    piece = (rows - direct, hidden // n_comm)
    scratch = [
        pltpu.VMEM((half - 1, 2) + block, bf16), pltpu.VMEM((half,) + block, bf16),
        pltpu.VMEM((n_comm, half) + piece, bf16), pltpu.VMEM((n_comm, half) + piece, bf16),
        pltpu.VMEM((half,) + piece, bf16), pltpu.VMEM((half,) + piece, bf16), pltpu.VMEM((n_comm,) + piece, bf16),
        pltpu.VMEM((rows - direct, hidden), bf16), pltpu.VMEM((rows - direct, hidden), bf16),
        dma((half,)), dma((half,)), dma((n_comm, half)), dma((n_comm, half)),
        dma((half,)), dma((half,)), dma((n_comm,)), dma((n_comm,)), dma((1,)), dma((1,)),
    ]
    if direct:
        scratch += [
            pltpu.VMEM((half, direct, hidden), bf16), pltpu.VMEM((half, direct, hidden), bf16),
            pltpu.VMEM((n_comm, direct, hidden), bf16), dma((half,)), dma((half,)), dma((n_comm,)), dma((n_comm,)),
        ]
    return pl.pallas_call(
        functools.partial(reduce_kernel, n_comm, n_wide, factor, column),
        out_shape=pltpu.VMEM(block, jnp.float32),
        in_specs=[pl.BlockSpec(memory_space=pltpu.VMEM)] * 3,
        out_specs=pl.BlockSpec(memory_space=pltpu.VMEM),
        scratch_shapes=scratch,
        compiler_params=pltpu.CompilerParams(
            collective_id=0, has_side_effects=True, vmem_limit_bytes=REDUCE_VMEM
        ),
        cost_estimate=pl.CostEstimate(flops=1 << 34, bytes_accessed=8 << 20, transcendentals=0),
    )(agg_t, new_dual, first)


def local(feats, tiles, tile_src, tile_count, request, z_old, dual, target, w_rows, rho, beta):
    own_count, nodes, _ = feats.shape
    hidden = w_rows.shape[1]
    n_comm = lax.axis_size("comm")
    n_wide = lax.axis_size("wide")
    part, agg_t, agg_last, w_last, scale, target, coef = step(
        tile_src, tile_count, request, feats, tiles, z_old, dual, target, w_rows,
        rho.reshape(1, hidden), beta.reshape(1, hidden), n_comm, n_wide,
    )
    new_z, new_dual, moved, first = finish(part, agg_t, agg_last, w_last, scale, target, coef, n_wide)
    factor = 1.0 / math.sqrt(own_count * nodes * n_comm * n_wide)
    return new_z, new_dual, reduce_grad(agg_t, moved, first, n_comm, n_wide, factor)


def solution(mesh):
    in_specs = (
        P(("comm", "wide"), None, None),
        P(("comm", "wide"), None, None, None),
        P(("comm", "wide"), None),
        P(("comm", "wide")),
        P(("comm", "wide"), None),
        P(("comm", "wide"), None, None),
        P(("comm", "wide"), None, None),
        P(("comm", "wide"), None, None),
        P("wide", None),
        P(),
        P(),
    )
    out_specs = (P(("comm", "wide"), None, None), P(("comm", "wide"), None, None), P("wide", None))
    return jax.shard_map(local, mesh=mesh, in_specs=in_specs, out_specs=out_specs, check_vma=False)
```

```python
import functools
import math

import jax
import jax.numpy as jnp
from jax import lax
from jax.experimental import pallas as pl
from jax.experimental.pallas import tpu as pltpu
from jax.sharding import PartitionSpec as P


STEP_VMEM = 40 * 1024 * 1024
FINISH_VMEM = 8 * 1024 * 1024
REDUCE_VMEM = 10 * 1024 * 1024

MESH = pl.DeviceIdType.MESH


def largest_block(size, limit, unit):
    for block in range(limit, 0, -unit):
        if size % block == 0:
            return block
    return size


def mxu(a, b):
    return jnp.dot(a, b, preferred_element_type=jnp.float32)


def signal(semaphore, to_c, to_w):
    pl.semaphore_signal(semaphore, inc=1, device_id=(to_c, to_w), device_id_type=MESH)


def enter(n_comm, n_wide, c, w, along):
    barrier = pltpu.get_barrier_semaphore()
    quick = n_comm == 4
    for off in (1, 2) if quick else range(1, n_comm):
        signal(barrier, lax.bitwise_xor(c, off) if quick else lax.rem(c + off, n_comm), w)
    greeted = 2 if quick else n_comm - 1
    if along:
        chip = w // 2
        last = n_wide // 2 - 1
        signal(barrier, c, w + 1 - 2 * lax.rem(w, 2))

        @pl.when(chip > 0)
        def _():
            signal(barrier, c, w - 2)

        @pl.when(chip < last)
        def _():
            signal(barrier, c, w + 2)

        greeted = greeted + 1 + jnp.minimum(chip, 1) + jnp.minimum(last - chip, 1)
    return greeted


def pass_on(n_comm, c, w, hello):
    if n_comm == 4:
        signal(hello.at[0], lax.bitwise_xor(c, 1), w)


def diagonal_is_in(n_comm, hello):
    if n_comm == 4:
        pl.semaphore_wait(hello.at[0], 1)


def far_are_in(n_wide, c, w, below, above):
    chip = w // 2
    last = n_wide // 2 - 1
    for far in range(1, last + 1):
        if far > 1:

            @pl.when(chip + far <= last)
            def _(far=far):
                pl.semaphore_wait(below.at[far - 1], 1)

            @pl.when(chip - far >= 0)
            def _(far=far):
                pl.semaphore_wait(above.at[far - 1], 1)

        if far < last:

            @pl.when(jnp.logical_and(chip + far <= last, chip > 0))
            def _(far=far):
                signal(below.at[far], c, w - 2)

            @pl.when(jnp.logical_and(chip - far >= 0, chip < last))
            def _(far=far):
                signal(above.at[far], c, w + 2)


def pieces_of(nodes, width):
    cw = largest_block(width, 256, 128)
    last = largest_block(nodes, 256, 128)
    early = 128 if cw == 256 and nodes > 128 and width > 2 * cw else 0
    pieces = [(0, early, early, nodes - early), (early, cw - early, 0, nodes)] if early else [(0, cw, 0, nodes)]
    pieces += [(j * cw, cw, 0, nodes) for j in range(1, width // cw - 1)]
    if last < nodes:
        pieces.append((width - cw, cw, 0, nodes - last))
    pieces.append((width - cw, cw, nodes - last if last < nodes else 0, last))
    return cw, early, pieces


def step_kernel(n_comm, n_wide, plan, *refs):
    (cw, early, pieces, rows, column, gather_w) = plan
    count = len(pieces)
    (src_hbm, count_hbm, request_hbm, feats_ref, tiles_ref, z_ref, dual_ref, target_ref, w_ref, rho_ref,
     beta_ref, part, agg_t, agg_last, w_last, scale, target, coef, src_ref, count_ref, request_ref, rates,
     own, tiles, dual, z_old, weight, held, ask, asked, eager) = refs[:31]
    pools = refs[31 : 31 + count]
    stages = refs[31 + count : 31 + 2 * count]
    (small_sem, own_sem, pool_sem, tile_sem, data_sem, w_sem, ask_send, ask_recv, feat_send, feat_recv,
     w_send, w_recv, fwd_send, fwd_recv, eager_sem, eager_send, eager_recv,
     hello, below, above) = refs[31 + 2 * count :]
    own_count, nodes, width = feats_ref.shape
    slots = tiles_ref.shape[1]
    hidden = w_ref.shape[-1]
    peers = n_comm - 1
    paired = n_comm & (n_comm - 1) == 0
    half = n_wide // 2
    dead = own_count + peers
    c = lax.axis_index("comm")
    w = lax.axis_index("wide")
    chip = w // 2
    side = lax.rem(w, 2)
    partner = w + 1 - 2 * side

    def towards(off):
        return lax.bitwise_xor(c, off) if paired else lax.rem(c + off, n_comm)

    def arriving(off):
        return lax.bitwise_xor(c, off) if paired else lax.rem(c - off + n_comm, n_comm)

    def along(off):
        return lax.rem(chip + off, half) * 2 + side

    def remote(src, dst, send, recv, to_c, to_w):
        return pltpu.make_async_remote_copy(
            src_ref=src, dst_ref=dst, send_sem=send, recv_sem=recv, device_id=(to_c, to_w),
            device_id_type=MESH,
        )

    def arrived(dst, recv):
        remote(dst, dst, recv, recv, c, partner).wait_recv()

    request_copy = pltpu.make_async_copy(request_hbm, request_ref, small_sem.at[0])
    request_copy.start()
    greeted = enter(n_comm, n_wide, c, w, gather_w)
    eager_copy = None
    if early:
        eager_copy = pltpu.make_async_copy(
            feats_ref.at[:, pl.ds(0, early), pl.ds(0, early)], eager.at[pl.ds(0, own_count)], eager_sem.at[0]
        )
        eager_copy.start()
    own_copy = pltpu.make_async_copy(feats_ref, own, own_sem.at[0])
    own_copy.start()
    w_copy = pltpu.make_async_copy(w_ref, weight.at[w] if gather_w else weight, w_sem.at[0])
    w_copy.start()
    small_copies = [
        pltpu.make_async_copy(src_hbm, src_ref, small_sem.at[1]),
        pltpu.make_async_copy(count_hbm, count_ref, small_sem.at[2]),
        pltpu.make_async_copy(rho_ref, rates.at[0], small_sem.at[3]),
        pltpu.make_async_copy(beta_ref, rates.at[1], small_sem.at[4]),
    ]
    pool_copies = [
        pltpu.make_async_copy(
            feats_ref.at[:, pl.ds(row, size), pl.ds(col, wide)], pools[p].at[pl.ds(0, own_count)], pool_sem.at[p]
        )
        for p, (col, wide, row, size) in enumerate(pieces)
    ]
    tile_copy = pltpu.make_async_copy(tiles_ref, tiles, tile_sem.at[0])
    data_copies = [
        pltpu.make_async_copy(dual_ref, dual, data_sem.at[0]),
        pltpu.make_async_copy(target_ref, target, data_sem.at[1]),
        pltpu.make_async_copy(z_ref, z_old, data_sem.at[2]),
    ]
    request_copy.wait()
    for off in range(1, n_comm):
        ask[off - 1] = jnp.full(ask.shape[1:], request_ref[0, arriving(off)], jnp.int32)
    pl.semaphore_wait(pltpu.get_barrier_semaphore(), greeted)

    started = []

    def start(*args):
        copy = remote(*args)
        copy.start()
        started.append(copy)

    near = list(range(1, peers)) + [peers]
    far = [peers] + list(range(1, peers))
    pass_on(n_comm, c, w, hello)

    def request(off):
        start(ask.at[off - 1], asked.at[off - 1], ask_send.at[off - 1], ask_recv.at[off - 1], arriving(off), w)

    def send_early(off):
        if early:
            start(
                eager.at[pl.ds(0, own_count)], eager.at[pl.ds(own_count * off, own_count)],
                eager_send.at[off - 1], eager_recv.at[off - 1], towards(off), w,
            )

    for off in near[:-1]:
        request(off)
    if early:
        eager_copy.wait()
    for off in near[:-1]:
        send_early(off)
    diagonal_is_in(n_comm, hello)
    request(peers)
    send_early(peers)
    for copy in small_copies + pool_copies + [tile_copy] + data_copies:
        copy.start()
    own_copy.wait()
    wants = {}
    for p, (col, wide, row, size) in enumerate(pieces):
        for off in near if p == 0 else far:
            if p == 0:
                arrived(asked.at[off - 1], ask_recv.at[off - 1])
                wants[off] = jnp.clip(jnp.max(asked[off - 1]), 0, own_count - 1)
            stages[p][off - 1] = own[wants[off], row : row + size, col : col + wide]
            start(
                stages[p].at[off - 1], pools[p].at[own_count + off - 1], feat_send.at[off - 1, p],
                feat_recv.at[off - 1, p], towards(off), w,
            )
    w_copy.wait()
    if gather_w:
        far_are_in(n_wide, c, w, below, above)
        for off in range(1, half):
            start(weight.at[w], weight.at[w], w_send.at[off - 1], w_recv.at[chip], c, along(off))
        start(weight.at[w], weight.at[w], fwd_send.at[0], fwd_recv.at[chip], c, partner)
    for p, (_, wide, _, size) in enumerate(pieces):
        pools[p][dead] = jnp.zeros((size, wide), jnp.bfloat16)
    if early:
        eager[own_count * n_comm] = jnp.zeros((early, early), jnp.bfloat16)
    for copy in small_copies:
        copy.wait()

    def pick(k, t):
        source = src_ref[k, t]
        member = jnp.maximum(source - own_count, 0)
        if paired:
            offset = lax.bitwise_xor(c, member)
        else:
            offset = lax.rem(c - member + n_comm, n_comm)
        other = jnp.where(member == c, request_ref[0, c], own_count + offset - 1)
        index = jnp.where(source < own_count, source, other)
        index = jnp.clip(index, 0, dead - 1)
        return jnp.where(t < count_ref[k], index, dead)

    def pick_eager(k, t):
        source = src_ref[k, t]
        member = jnp.clip(source - own_count, 0, peers)
        if paired:
            offset = lax.bitwise_xor(c, member)
        else:
            offset = lax.rem(c - member + n_comm, n_comm)
        index = jnp.where(source < own_count, source, own_count * offset + request_ref[0, member])
        index = jnp.clip(index, 0, own_count * n_comm - 1)
        return jnp.where(t < count_ref[k], index, own_count * n_comm)

    rho = rates[0]
    beta = rates[1]
    inverse = 1.0 / rho
    blend = beta / (rho + beta)
    gain = rho * blend
    coef[0:1] = inverse

    def products(p, k, block):
        (_, _, row, size) = pieces[p]
        total = mxu(tiles[k, 0, block, row : row + size], pools[p][pick(k, 0)])
        for t in range(1, slots):
            total = total + mxu(tiles[k, t, block, row : row + size], pools[p][pick(k, t)])
        if early and p == 0:
            for t in range(slots):
                total = total + mxu(tiles[k, t, block, :early], eager[pick_eager(k, t)])
        return total

    if gather_w:
        for off in range(1, half):
            other = along(off)
            arrived(weight.at[other], w_recv.at[other // 2])
            start(weight.at[other], weight.at[other], fwd_send.at[off], fwd_recv.at[other // 2], c, partner)
        for at in range(half):
            arrived(weight.at[at * 2 + 1 - side], fwd_recv.at[at])
    tile_copy.wait()
    for copy in data_copies:
        copy.wait()

    def w_rows_of(col, wide, cols):
        if gather_w:
            return weight[...].reshape(width, hidden)[col : col + wide, cols]
        return weight[col : col + wide, cols]

    for at in range(hidden // column):
        cols = slice(at * column, (at + 1) * column)
        w_last[:, cols] = w_rows_of(width - cw, cw, cols)

    for p, (col, wide, row, size) in enumerate(pieces):
        pool_copies[p].wait()
        if early and p == 0:
            for off in far:
                arrived(eager.at[pl.ds(own_count * off, own_count)], eager_recv.at[off - 1])
        for off in far:
            arrived(pools[p].at[own_count + off - 1], feat_recv.at[off - 1, p])
        if p == count - 1:
            for k in range(own_count):
                for step in range(nodes // rows):
                    block = slice(step * rows, (step + 1) * rows)
                    total = products(p, k, block)
                    if size < nodes:
                        total = total + held[k, block]
                    agg = total.astype(jnp.bfloat16)
                    agg_last[k, block] = agg
                    at = k * nodes + step * rows
                    agg_t[col : col + cw, at : at + rows] = agg.T
            continue
        steps = nodes // rows

        def body(step, carry, p=p, col=col, wide=wide, steps=steps):
            k = step // steps
            at = lax.rem(step, steps)
            block = pl.ds(pl.multiple_of(at * rows, rows), rows)
            total = products(p, k, block)
            if col == width - cw:
                held[k, block] = total
                return carry
            if p == 0:
                for n in range(hidden // column):
                    cols = slice(n * column, (n + 1) * column)
                    active = z_old[k, block, cols].astype(jnp.float32) > 0
                    scale[k, block, cols] = jnp.where(active, jnp.broadcast_to(gain[:, cols], active.shape), 0.0)
            agg = total.astype(jnp.bfloat16)
            agg_t[col : col + wide, pl.ds(pl.multiple_of(k * nodes + at * rows, 128), rows)] = agg.T
            for n in range(hidden // column):
                cols = slice(n * column, (n + 1) * column)
                value = mxu(agg, w_rows_of(col, wide, cols))
                if p == 0:
                    value = value + (
                        dual[k, block, cols].astype(jnp.float32) * inverse[:, cols]
                        - target[k, block, cols].astype(jnp.float32)
                    )
                else:
                    value = value + part[k, block, cols]
                part[k, block, cols] = value
            return carry

        lax.fori_loop(0, own_count * steps, body, 0)
    for copy in started:
        copy.wait_send()


def step(tile_src, tile_count, request, feats, tiles, z_old, dual, target, w_rows, rho, beta, n_comm, n_wide):
    own_count, nodes, width = feats.shape
    hidden = w_rows.shape[1]
    gather_w = w_rows.shape[0] % 16 == 0
    if not gather_w:
        w_rows = lax.all_gather(w_rows, "wide", axis=0, tiled=True)
    cw, early, pieces = pieces_of(nodes, width)
    column = largest_block(hidden, 256, 128)
    rows = largest_block(nodes, 384, 128)
    plan = (cw, early, pieces, rows, column, gather_w)
    peers = n_comm - 1
    half = n_wide // 2
    count = len(pieces)
    bf16 = jnp.bfloat16
    f32 = jnp.float32
    regular = pltpu.SemaphoreType.REGULAR
    dma = pltpu.SemaphoreType.DMA
    weight = pltpu.VMEM((n_wide,) + w_rows.shape if gather_w else w_rows.shape, bf16)
    return pl.pallas_call(
        functools.partial(step_kernel, n_comm, n_wide, plan),
        out_shape=[
            pltpu.VMEM(z_old.shape, f32),
            pltpu.VMEM((width, own_count * nodes), bf16),
            pltpu.VMEM((own_count, nodes, cw), bf16),
            pltpu.VMEM((cw, hidden), bf16),
            pltpu.VMEM(z_old.shape, f32),
            pltpu.VMEM(target.shape, bf16),
            pltpu.VMEM((1, hidden), f32),
        ],
        in_specs=[pl.BlockSpec(memory_space=pl.ANY)] * 11,
        out_specs=[pl.BlockSpec(memory_space=pltpu.VMEM)] * 7,
        scratch_shapes=[
            pltpu.SMEM(tile_src.shape, jnp.int32),
            pltpu.SMEM(tile_count.shape, jnp.int32),
            pltpu.SMEM(request.shape, jnp.int32),
            pltpu.VMEM((2, 1, hidden), f32),
            pltpu.VMEM(feats.shape, bf16),
            pltpu.VMEM(tiles.shape, bf16),
            pltpu.VMEM(dual.shape, bf16),
            pltpu.VMEM(z_old.shape, bf16),
            weight,
            pltpu.VMEM((own_count, nodes, cw), f32),
            pltpu.VMEM((peers, 8, 128), jnp.int32),
            pltpu.VMEM((peers, 8, 128), jnp.int32),
            pltpu.VMEM((own_count * n_comm + 1, max(early, 16), max(early, 128)), bf16),
        ]
        + [pltpu.VMEM((own_count + n_comm, size, wide), bf16) for (_, wide, _, size) in pieces]
        + [pltpu.VMEM((peers, size, wide), bf16) for (_, wide, _, size) in pieces]
        + [
            dma((5,)), dma((1,)), dma((count,)), dma((1,)), dma((3,)), dma((1,)), dma((peers,)), dma((peers,)),
            dma((peers, count)), dma((peers, count)), dma((half,)), dma((half,)), dma((half,)), dma((half,)),
            dma((1,)), dma((peers,)), dma((peers,)), regular((1,)), regular((half,)), regular((half,)),
        ],
        compiler_params=pltpu.CompilerParams(
            collective_id=1, has_side_effects=True, vmem_limit_bytes=STEP_VMEM
        ),
        cost_estimate=pl.CostEstimate(flops=1 << 36, bytes_accessed=32 << 20, transcendentals=0),
    )(tile_src, tile_count, request, feats, tiles, z_old, dual, target, w_rows, rho, beta)


def finish_kernel(
    n_wide, rows, column, part, agg_t, agg_last, w_last, scale, target, coef, newz_ref, newdual_ref, moved_ref,
    grads, newz, sems,
):
    own_count, nodes, hidden = part.shape
    inverse = coef[...]
    copies = []
    for k in range(own_count):
        for step in range(nodes // rows):
            block = slice(step * rows, (step + 1) * rows)
            agg = agg_last[k, block]
            for n in range(hidden // column):
                cols = slice(n * column, (n + 1) * column)
                gap = mxu(agg, w_last[:, cols]) + part[k, block, cols]
                moved = gap * scale[k, block, cols]
                moved_ref[k, block, cols] = moved.astype(jnp.bfloat16)
                newz[k, block, cols] = (
                    gap + target[k, block, cols].astype(jnp.float32) - moved * inverse[:, cols]
                ).astype(jnp.bfloat16)
            for src, dst in ((newz, newz_ref), (moved_ref, newdual_ref)):
                copy = pltpu.make_async_copy(src.at[k, block], dst.at[k, block], sems.at[len(copies)])
                copy.start()
                copies.append(copy)
    j = jnp.where(lax.axis_index("wide") // 2 == 0, 1, 0)
    gradient(agg_t, moved_ref, grads, j, column)
    for copy in copies:
        copy.wait()


def gradient(agg_t, moved_ref, grads, j, column):
    own_count, nodes, hidden = moved_ref.shape
    _, shard, _ = grads.shape
    block = slice(0, 2 * shard) if isinstance(j, int) else pl.ds(pl.multiple_of(j * (2 * shard), 2 * shard), 2 * shard)
    for n in range(hidden // column):
        cols = slice(n * column, (n + 1) * column)
        moved = moved_ref[:, :, cols].reshape(own_count * nodes, column)
        value = mxu(agg_t[block, :], moved).astype(jnp.bfloat16)
        grads[0, :, cols] = value[:shard]
        grads[1, :, cols] = value[shard:]


def finish(part, agg_t, agg_last, w_last, scale, target, coef, n_wide):
    own_count, nodes, hidden = part.shape
    width = agg_t.shape[0]
    rows = largest_block(nodes, 256, 128)
    column = largest_block(hidden, 256, 128)
    vmem = pl.BlockSpec(memory_space=pltpu.VMEM)
    anywhere = pl.BlockSpec(memory_space=pl.ANY)
    bf16 = jnp.bfloat16
    return pl.pallas_call(
        functools.partial(finish_kernel, n_wide, rows, column),
        out_shape=[
            jax.ShapeDtypeStruct(part.shape, bf16),
            jax.ShapeDtypeStruct(part.shape, bf16),
            pltpu.VMEM(part.shape, bf16),
            pltpu.VMEM((2, width // n_wide, hidden), bf16),
        ],
        in_specs=[vmem] * 7,
        out_specs=[pl.BlockSpec(memory_space=pltpu.HBM)] * 2 + [vmem] * 2,
        scratch_shapes=[
            pltpu.VMEM(part.shape, bf16),
            pltpu.SemaphoreType.DMA((2 * own_count * (nodes // rows),)),
        ],
        compiler_params=pltpu.CompilerParams(vmem_limit_bytes=FINISH_VMEM),
        cost_estimate=pl.CostEstimate(flops=1 << 32, bytes_accessed=8 << 20, transcendentals=0),
    )(part, agg_t, agg_last, w_last, scale, target, coef)


def direct_rows(rows):
    return 16 if rows % 16 == 0 and rows >= 64 else 0


def reduce_kernel(n_comm, n_wide, factor, column, agg_ref, dual_ref, first_ref, out_ref, *refs):
    half = n_wide // 2
    shard, hidden = out_ref.shape
    direct = direct_rows(shard)
    (grads, got_pair, sums, got_comm, parts, got_wide, final, early_own, early_got, pair_send, pair_recv, comm_send, comm_recv,
     wide_send, wide_recv, final_send, final_recv, early_send, early_recv) = refs[:19]
    if direct:
        whole_own, whole_got, whole, direct_send, direct_recv, whole_send, whole_recv = refs[19:]
    size = shard - direct
    columns = hidden // n_comm
    c = lax.axis_index("comm")
    w = lax.axis_index("wide")
    mine = w // 2
    side = lax.rem(w, 2)
    partner = w + 1 - 2 * side
    paired = n_comm & (n_comm - 1) == 0
    even = half & (half - 1) == 0
    lead = mine == 0
    follow = mine != 0

    def signal(to_c, to_w):
        pl.semaphore_signal(
            pltpu.get_barrier_semaphore(), inc=1, device_id=(to_c, to_w), device_id_type=MESH
        )

    signal(c, partner)
    for off in range(1, half):
        signal(c, lax.rem(mine + off, half) * 2 + side)
    for off in range(1, n_comm):
        signal(lax.rem(c + off, n_comm), w)

    def remote(src, dst, send, recv, to_c, to_w):
        return pltpu.make_async_remote_copy(
            src_ref=src, dst_ref=dst, send_sem=send, recv_sem=recv, device_id=(to_c, to_w),
            device_id_type=MESH,
        )

    def arrived(dst, recv):
        remote(dst, dst, recv, recv, c, partner).wait_recv()

    started = []

    def start(*args, when=None):
        copy = remote(*args)
        started.append((copy, when))
        if when is None:
            copy.start()
        else:
            pl.when(when)(copy.start)

    def towards(off):
        return lax.bitwise_xor(c, off) if paired else lax.rem(c + off, n_comm)

    def across(off):
        return lax.bitwise_xor(mine, off) if even else lax.rem(mine + off, half)

    place = half - 1 - mine if even else mine - 1
    listed = [across(off) for off in range(half - 1, 0, -1)] + [mine]
    order = [0] + [jnp.where(at - 1 < place, listed[at - 1], listed[at]) for at in range(1, half)]
    leading = [listed[half - 2]] + listed[: half - 2] + [mine]
    order = [jnp.where(lead, leading[at], order[at]) for at in range(half)]
    far = [n_comm - 1] + list(range(1, n_comm - 1))

    def partial(at):
        return first_ref if at == 0 else grads.at[at - 1]

    def combine(at):
        arrived(got_pair.at[at], pair_recv.at[at])
        value = partial(at)[side].astype(jnp.float32) + got_pair[at].astype(jnp.float32)
        head = value[:size]
        if at == half - 1:

            @pl.when(mine == 1)
            def _():
                arrived(early_got, early_recv.at[0])

            head = head + early_got[...].astype(jnp.float32)
        head = head.astype(jnp.bfloat16)
        for q in range(n_comm):
            sums[q, at] = head[:, q * columns : (q + 1) * columns]
        for off in far:
            start(
                sums.at[towards(off), at], got_comm.at[c, at], comm_send.at[off - 1, at],
                comm_recv.at[c, at], towards(off), w, when=follow if at == 0 else None,
            )
        if at == 0:
            early_own[...] = head
            start(early_own, early_got, early_send.at[0], early_recv.at[0], c, 2 + side, when=lead)
        if direct:
            whole_own[at] = value[size:].astype(jnp.bfloat16)
            if at < half - 1:
                start(
                    whole_own.at[at], whole_got.at[mine], direct_send.at[at], direct_recv.at[mine],
                    c, order[at] * 2 + side,
                )

    @pl.when(mine != 1)
    def _():
        early_got[...] = jnp.zeros_like(early_got)

    @pl.when(mine == 1)
    def _():
        got_wide[0] = jnp.zeros(got_wide.shape[1:], jnp.bfloat16)

    pl.semaphore_wait(pltpu.get_barrier_semaphore(), 1 + (half - 1) + (n_comm - 1))
    for at, j in enumerate(order):
        if at > 0:
            gradient(agg_ref, dual_ref, grads.at[at - 1], j, column)
        start(
            partial(at).at[1 - side], got_pair.at[at], pair_send.at[at], pair_recv.at[at], c, partner
        )
        if at > 0:
            combine(at - 1)

    finals = [
        remote(final.at[c], final.at[c], final_send.at[off - 1], final_recv.at[c], towards(off), w) for off in far
    ]

    def received(at):
        value = sums[c, at].astype(jnp.float32)
        for off in far:
            q = towards(off)
            arrived(got_comm.at[q, at], comm_recv.at[q, at])
            value = value + got_comm[q, at].astype(jnp.float32)
        return value

    wides = [
        remote(parts.at[at], got_wide.at[mine], wide_send.at[at], wide_recv.at[mine], c, order[at] * 2 + side)
        for at in range(half - 1)
    ]

    def forward(at):
        parts[at] = received(at).astype(jnp.bfloat16)
        wides[at].start()

    for at in range(half - 1):
        if at == 0:
            pl.when(follow)(functools.partial(forward, 0))
            combine(half - 1)
        else:
            forward(at)
        if direct and at == 0:
            total = whole_own[half - 1].astype(jnp.float32)
            for off in range(1, half):
                other = across(off)
                arrived(whole_got.at[other], direct_recv.at[other])
                total = total + whole_got[other].astype(jnp.float32)
            whole[c] = total.astype(jnp.bfloat16)
            for off in far:
                start(whole.at[c], whole.at[c], whole_send.at[off - 1], whole_recv.at[c], towards(off), w)
    total = received(half - 1)
    for off in range(1, half):
        other = across(off)

        @pl.when(jnp.logical_not(jnp.logical_and(mine == 1, other == 0)))
        def _(other=other):
            arrived(got_wide.at[other], wide_recv.at[other])

        total = total + got_wide[other].astype(jnp.float32)
    final[c] = total.astype(jnp.bfloat16)
    for copy in finals:
        copy.start()
    if direct:
        for off in far:
            arrived(whole.at[towards(off)], whole_recv.at[towards(off)])
        total = whole[0].astype(jnp.float32)
        for q in range(1, n_comm):
            total = total + whole[q].astype(jnp.float32)
        out_ref[size:] = total * factor
    for off in far:
        arrived(final.at[towards(off)], final_recv.at[towards(off)])
    for q in range(n_comm):
        out_ref[:size, q * columns : (q + 1) * columns] = final[q].astype(jnp.float32) * factor
    waits = started + [(copy, None) for copy in finals]
    waits += [(copy, follow if at == 0 else None) for at, copy in enumerate(wides)]
    for copy, when in waits:
        if when is None:
            copy.wait_send()
        else:
            pl.when(when)(copy.wait_send)


def reduce_grad(agg_t, new_dual, first, n_comm, n_wide, factor):
    width = agg_t.shape[0]
    hidden = new_dual.shape[2]
    rows = width // n_wide
    half = n_wide // 2
    block = (rows, hidden)
    column = largest_block(hidden, 256, 128)
    bf16 = jnp.bfloat16
    dma = pltpu.SemaphoreType.DMA
    direct = direct_rows(rows)
    piece = (rows - direct, hidden // n_comm)
    scratch = [
        pltpu.VMEM((half - 1, 2) + block, bf16), pltpu.VMEM((half,) + block, bf16),
        pltpu.VMEM((n_comm, half) + piece, bf16), pltpu.VMEM((n_comm, half) + piece, bf16),
        pltpu.VMEM((half,) + piece, bf16), pltpu.VMEM((half,) + piece, bf16), pltpu.VMEM((n_comm,) + piece, bf16),
        pltpu.VMEM((rows - direct, hidden), bf16), pltpu.VMEM((rows - direct, hidden), bf16),
        dma((half,)), dma((half,)), dma((n_comm, half)), dma((n_comm, half)),
        dma((half,)), dma((half,)), dma((n_comm,)), dma((n_comm,)), dma((1,)), dma((1,)),
    ]
    if direct:
        scratch += [
            pltpu.VMEM((half, direct, hidden), bf16), pltpu.VMEM((half, direct, hidden), bf16),
            pltpu.VMEM((n_comm, direct, hidden), bf16), dma((half,)), dma((half,)), dma((n_comm,)), dma((n_comm,)),
        ]
    return pl.pallas_call(
        functools.partial(reduce_kernel, n_comm, n_wide, factor, column),
        out_shape=pltpu.VMEM(block, jnp.float32),
        in_specs=[pl.BlockSpec(memory_space=pltpu.VMEM)] * 3,
        out_specs=pl.BlockSpec(memory_space=pltpu.VMEM),
        scratch_shapes=scratch,
        compiler_params=pltpu.CompilerParams(
            collective_id=0, has_side_effects=True, vmem_limit_bytes=REDUCE_VMEM
        ),
        cost_estimate=pl.CostEstimate(flops=1 << 34, bytes_accessed=8 << 20, transcendentals=0),
    )(agg_t, new_dual, first)


def local(feats, tiles, tile_src, tile_count, request, z_old, dual, target, w_rows, rho, beta):
    own_count, nodes, _ = feats.shape
    hidden = w_rows.shape[1]
    n_comm = lax.axis_size("comm")
    n_wide = lax.axis_size("wide")
    part, agg_t, agg_last, w_last, scale, target, coef = step(
        tile_src, tile_count, request, feats, tiles, z_old, dual, target, w_rows,
        rho.reshape(1, hidden), beta.reshape(1, hidden), n_comm, n_wide,
    )
    new_z, new_dual, moved, first = finish(part, agg_t, agg_last, w_last, scale, target, coef, n_wide)
    factor = 1.0 / math.sqrt(own_count * nodes * n_comm * n_wide)
    return new_z, new_dual, reduce_grad(agg_t, moved, first, n_comm, n_wide, factor)


def solution(mesh):
    in_specs = (
        P(("comm", "wide"), None, None),
        P(("comm", "wide"), None, None, None),
        P(("comm", "wide"), None),
        P(("comm", "wide")),
        P(("comm", "wide"), None),
        P(("comm", "wide"), None, None),
        P(("comm", "wide"), None, None),
        P(("comm", "wide"), None, None),
        P("wide", None),
        P(),
        P(),
    )
    out_specs = (P(("comm", "wide"), None, None), P(("comm", "wide"), None, None), P("wide", None))
    return jax.shard_map(local, mesh=mesh, in_specs=in_specs, out_specs=out_specs, check_vma=False)
```
